8 devices in a mesh: pool: 8 (over z, y, x, core).
Axes of the slice: x: 2, y: 2, z: 1, core: 2. Of those that a mesh axis runs over, the one named last changes fastest.
Arguments:
- hidden: bfloat16 [8, 64, 2048], P('pool')
- prefix_len: int32 [8], P('pool')
- prefix_table: int32 [8, 256, 2], P('pool')
- write_table: int32 [8, 1, 2], P('pool')
- cache_c: bfloat16 [8, 5, 64, 512], P('pool')
- cache_kr: bfloat16 [8, 5, 64, 64], P('pool')
- w_q: bfloat16 [2048, 3072], replicated
- w_dkv: bfloat16 [2048, 576], replicated
- g_kv: bfloat16 [512], replicated
- w_uk: bfloat16 [512, 16, 128], replicated
- w_uv: bfloat16 [512, 16, 128], replicated
- w_o: bfloat16 [2048, 2048], replicated
Outputs:
- output 1: bfloat16 [8, 64, 2048], P('pool')
- output 2: bfloat16 [8, 5, 64, 512], P('pool')
- output 3: bfloat16 [8, 5, 64, 64], P('pool')
All inputs are finite; a program needn't handle non-finite values.
Results may differ from the reference program's by a relative error of at most 0.00713187.
Values are sent between devices in bfloat16 or wider.
A program may use at most 1 GiB of HBM per device.

```python
import math
import jax
import jax.numpy as jnp
from jax import lax

POOL_SIZE = 8
REQ_DEV = 1
CHUNK_LEN = 64
PREFIX_MAX = 16384
PREFIX_PAGES = 4
D_MODEL = 2048
NUM_HEADS = 16
PAGE_LEN = 64
LATENT = 512
ROPE_DIM = 64
NOPE_DIM = 128
VALUE_DIM = 128

REQUESTS = POOL_SIZE * REQ_DEV
TABLE_PAGES = PREFIX_MAX // PAGE_LEN
CHUNK_PAGES = CHUNK_LEN // PAGE_LEN
CACHE_PAGES = PREFIX_PAGES + REQ_DEV * CHUNK_PAGES
READ_SLOTS = max(1, (2 * REQ_DEV * TABLE_PAGES) // POOL_SIZE)
NORM_EPS = 1e-6
ROPE_BASE = 10000.0


def rope_tables(positions):
    half_dim = ROPE_DIM // 2
    inv_freq = ROPE_BASE ** (-jnp.arange(half_dim, dtype=jnp.float32) / half_dim)
    angles = positions.astype(jnp.float32)[..., None] * inv_freq
    return jnp.cos(angles), jnp.sin(angles)


def apply_rope(values, cos_tab, sin_tab):
    half_dim = ROPE_DIM // 2
    first = values[..., :half_dim]
    second = values[..., half_dim:]
    return jnp.concatenate([first * cos_tab - second * sin_tab, second * cos_tab + first * sin_tab], axis=-1)


def draw_tables(key):
    key_len, key_perm, key_rot, key_page, key_write = jax.random.split(key, 5)
    req_ids = jnp.arange(REQUESTS)
    page_counts = jax.random.randint(key_len, (REQUESTS,), 0, TABLE_PAGES + 1)
    page_counts = jnp.where(req_ids == 0, TABLE_PAGES, jnp.where(req_ids == REQUESTS - 1, 0, page_counts))
    prefix_len = (page_counts * PAGE_LEN).astype(jnp.int32)
    is_valid = (jnp.arange(TABLE_PAGES)[None, :] < page_counts[:, None]).reshape(POOL_SIZE, REQ_DEV * TABLE_PAGES)
    slot_rank = jnp.cumsum(is_valid.astype(jnp.int32), axis=1) - 1
    owner_perm = jax.random.permutation(key_perm, POOL_SIZE)
    rotation = jax.random.randint(key_rot, (POOL_SIZE, 1), 0, max(1, POOL_SIZE // 4))
    owners = owner_perm[(rotation + slot_rank // READ_SLOTS) % POOL_SIZE]
    page_pick = jax.random.randint(key_page, (POOL_SIZE, REQ_DEV * TABLE_PAGES), 0, PREFIX_PAGES)
    prefix_table = jnp.stack([jnp.where(is_valid, owners, -1), jnp.where(is_valid, page_pick, -1)], axis=-1)
    prefix_table = prefix_table.reshape(REQUESTS, TABLE_PAGES, 2).astype(jnp.int32)
    write_ids = jnp.arange(REQ_DEV * CHUNK_PAGES)
    offsets = jax.random.permutation(key_write, POOL_SIZE)[write_ids % POOL_SIZE]
    write_owner = (jnp.arange(POOL_SIZE)[:, None] + offsets[None, :]) % POOL_SIZE
    write_page = jnp.broadcast_to(PREFIX_PAGES + write_ids[None, :], (POOL_SIZE, REQ_DEV * CHUNK_PAGES))
    write_table = jnp.stack([write_owner, write_page], axis=-1).reshape(REQUESTS, CHUNK_PAGES, 2).astype(jnp.int32)
    return prefix_len, prefix_table, write_table


def setup_inputs(seed: int = 0) -> dict:
    key_list = jax.random.split(jax.random.key(seed), 12)
    prefix_len, prefix_table, write_table = draw_tables(key_list[0])
    q_gain = math.sqrt(math.log((PREFIX_MAX + CHUNK_LEN) / 8.0) / 3.0)
    hidden = jax.random.normal(key_list[1], (REQUESTS, CHUNK_LEN, D_MODEL), jnp.float32)
    cache_c = jax.random.normal(key_list[2], (POOL_SIZE, CACHE_PAGES, PAGE_LEN, LATENT), jnp.float32)
    cache_kr = jax.random.normal(key_list[3], (POOL_SIZE, CACHE_PAGES, PAGE_LEN, ROPE_DIM), jnp.float32)
    w_q = jax.random.normal(key_list[4], (D_MODEL, NUM_HEADS * (NOPE_DIM + ROPE_DIM)), jnp.float32) * (q_gain / math.sqrt(D_MODEL))
    w_dkv = jax.random.normal(key_list[5], (D_MODEL, LATENT + ROPE_DIM), jnp.float32) / math.sqrt(D_MODEL)
    g_kv = jax.random.uniform(key_list[6], (LATENT,), jnp.float32, 0.5, 1.5)
    w_uk = jax.random.normal(key_list[7], (LATENT, NUM_HEADS, NOPE_DIM), jnp.float32) / math.sqrt(NOPE_DIM)
    w_uv = jax.random.normal(key_list[8], (LATENT, NUM_HEADS, VALUE_DIM), jnp.float32) / math.sqrt(LATENT)
    w_o = jax.random.normal(key_list[9], (NUM_HEADS * VALUE_DIM, D_MODEL), jnp.float32) / math.sqrt(NUM_HEADS * VALUE_DIM)
    return {
        "hidden": hidden.astype(jnp.bfloat16),
        "prefix_len": prefix_len,
        "prefix_table": prefix_table,
        "write_table": write_table,
        "cache_c": cache_c.astype(jnp.bfloat16),
        "cache_kr": cache_kr.astype(jnp.bfloat16),
        "w_q": w_q.astype(jnp.bfloat16),
        "w_dkv": w_dkv.astype(jnp.bfloat16),
        "g_kv": g_kv.astype(jnp.bfloat16),
        "w_uk": w_uk.astype(jnp.bfloat16),
        "w_uv": w_uv.astype(jnp.bfloat16),
        "w_o": w_o.astype(jnp.bfloat16),
    }


def reference(hidden, prefix_len, prefix_table, write_table, cache_c, cache_kr, w_q, w_dkv, g_kv, w_uk, w_uv, w_o):
    flat_c = cache_c.reshape(POOL_SIZE * CACHE_PAGES, PAGE_LEN, LATENT)
    flat_kr = cache_kr.reshape(POOL_SIZE * CACHE_PAGES, PAGE_LEN, ROPE_DIM)
    score_scale = (NOPE_DIM + ROPE_DIM) ** -0.5
    w_uk32 = w_uk.astype(jnp.float32)
    w_uv32 = w_uv.astype(jnp.float32)
    kv_gain = g_kv.astype(jnp.float32)
    query_ids = jnp.arange(CHUNK_LEN)
    key_ids = jnp.arange(PREFIX_MAX + CHUNK_LEN)

    def one_request(req_item):
        x_req, pre_len, req_table = req_item
        page_ids = jnp.maximum(req_table[:, 0], 0) * CACHE_PAGES + jnp.maximum(req_table[:, 1], 0)
        pre_c = flat_c[page_ids].reshape(PREFIX_MAX, LATENT)
        pre_kr = flat_kr[page_ids].reshape(PREFIX_MAX, ROPE_DIM)
        q_all = jnp.dot(x_req, w_q, preferred_element_type=jnp.float32).astype(jnp.bfloat16)
        q_all = q_all.reshape(CHUNK_LEN, NUM_HEADS, NOPE_DIM + ROPE_DIM)
        kv_lat = jnp.dot(x_req, w_dkv, preferred_element_type=jnp.float32)
        lat_part = kv_lat[:, :LATENT]
        inv_rms = lax.rsqrt(jnp.mean(lat_part * lat_part, axis=-1, keepdims=True) + NORM_EPS)
        c_new = (lat_part * inv_rms * kv_gain).astype(jnp.bfloat16)
        cos_tab, sin_tab = rope_tables(pre_len + query_ids)
        kr_new = apply_rope(kv_lat[:, LATENT:], cos_tab, sin_tab).astype(jnp.bfloat16)
        q_rope = apply_rope(q_all[:, :, NOPE_DIM:].astype(jnp.float32), cos_tab[:, None, :], sin_tab[:, None, :]).astype(jnp.bfloat16)
        q_lat = jnp.einsum("chn,lhn->chl", q_all[:, :, :NOPE_DIM].astype(jnp.float32), w_uk32).astype(jnp.bfloat16)
        keys_c = jnp.concatenate([pre_c, c_new], axis=0).astype(jnp.float32)
        keys_r = jnp.concatenate([pre_kr, kr_new], axis=0).astype(jnp.float32)
        scores = jnp.einsum("chl,jl->hcj", q_lat.astype(jnp.float32), keys_c)
        scores = (scores + jnp.einsum("chr,jr->hcj", q_rope.astype(jnp.float32), keys_r)) * score_scale
        visible = jnp.where(key_ids[None, :] < PREFIX_MAX, key_ids[None, :] < pre_len, key_ids[None, :] - PREFIX_MAX <= query_ids[:, None])
        scores = jnp.where(visible[None, :, :], scores, -jnp.inf)
        weights = jax.nn.softmax(scores, axis=-1)
        o_lat = jnp.einsum("hcj,jl->chl", weights, keys_c).astype(jnp.bfloat16)
        o_heads = jnp.einsum("chl,lhv->chv", o_lat.astype(jnp.float32), w_uv32).astype(jnp.bfloat16)
        attn_out = jnp.dot(o_heads.reshape(CHUNK_LEN, NUM_HEADS * VALUE_DIM), w_o, preferred_element_type=jnp.float32)
        y_req = (x_req.astype(jnp.float32) + attn_out).astype(jnp.bfloat16)
        return y_req, c_new, kr_new

    hidden_out, new_c, new_kr = lax.map(one_request, (hidden, prefix_len, prefix_table))
    dest_rows = (write_table[:, :, 0] * CACHE_PAGES + write_table[:, :, 1]).reshape(REQUESTS * CHUNK_PAGES)
    cache_c_out = flat_c.at[dest_rows].set(new_c.reshape(REQUESTS * CHUNK_PAGES, PAGE_LEN, LATENT))
    cache_kr_out = flat_kr.at[dest_rows].set(new_kr.reshape(REQUESTS * CHUNK_PAGES, PAGE_LEN, ROPE_DIM))
    cache_c_out = cache_c_out.reshape(POOL_SIZE, CACHE_PAGES, PAGE_LEN, LATENT)
    cache_kr_out = cache_kr_out.reshape(POOL_SIZE, CACHE_PAGES, PAGE_LEN, ROPE_DIM)
    return hidden_out, cache_c_out, cache_kr_out
```

```python
import functools
import math

import jax
import jax.numpy as jnp
import numpy as np
from jax import lax
from jax.experimental import pallas as pl
from jax.experimental.pallas import tpu as pltpu
from jax.sharding import PartitionSpec as P

BF = jnp.bfloat16
F32 = jnp.float32
MESH = pl.DeviceIdType.MESH

TOK = 64
DM = 2048
NH = 16
LAT = 512
RD = 64
ND = 128
HQ = ND + RD
ROWS = NH * TOK
EPS = 1e-6
GROUP = 4
GCOLS = GROUP * HQ
NGROUP = NH // GROUP
BLK = 256
SCALE2 = float((ND + RD) ** -0.5 * math.log2(math.e))
INV_FREQ = [float(np.float32(10000.0 ** (-k / 32.0))) for k in range(32)]

CHUNKS = (
    ((0, 0), (0, 1)),
    ((1, 0), (1, 1)),
    ((2, 0), (4, 1)),
    ((3, 0), (5, 1)),
    ((2, 1), (4, 0)),
    ((3, 1), (5, 0)),
    ((6, 0), (6, 1)),
    ((7, 0), (7, 1)),
)

FLOWS = {
    "x0": (0, 0, 2, 0, "x"),
    "x1": (0, 1, 4, 0, "x"),
    "y1": (0, 1, 2, 1, "y"),
    "y0": (0, 0, 4, 1, "y"),
    "p0": (0, 0, 1, 0, "p"),
    "p1": (0, 1, 1, 1, "p"),
    "dy": (2, 0, 6, 0, "y"),
    "dx": (2, 1, 6, 1, "x"),
    "p20": (2, 0, 3, 0, "p"),
    "p21": (2, 1, 3, 1, "p"),
    "p40": (4, 0, 5, 0, "p"),
    "p41": (4, 1, 5, 1, "p"),
    "p60": (6, 0, 7, 0, "p"),
    "p61": (6, 1, 7, 1, "p"),
}
FLOW_ID = {name: i for i, name in enumerate(FLOWS)}
NF = 2 * len(FLOWS)

NEWS = {
    "nx": (0, 2, "x", (0, 1), True),
    "ny": (0, 4, "y", (0, 1), True),
    "np": (0, 1, "p", (0, 1), True),
    "n2p": (2, 3, "p", (0, 1), True),
    "n4p": (4, 5, "p", (0, 1), True),
    "ndy": (2, 6, "y", (0,), False),
    "ndx": (4, 6, "x", (1,), True),
    "n6p": (6, 7, "p", (0, 1), True),
}
NEW_ID = {}
for _name, (_s, _t, _d, _h, _k) in NEWS.items():
    for _part in ("c", "k"):
        if _part == "c" or _k:
            NEW_ID[(_name, _part)] = NF + len(NEW_ID)
NSEM = NF + len(NEW_ID)


def body(x_hbm, plen_hbm, tbl_hbm, wt_hbm, cc_hbm, ckr_hbm, wq_hbm, wdkv_hbm, g_hbm, wuk_hbm, wuv_hbm, wo_hbm,
         y_hbm, cco_hbm, ckro_hbm,
         x_v, plen_s, tbl_v, wt_s, ckr_v, wq_v, wdkv_v, g_v, wuk_v, wuv_v, wo_v,
         kc, krp, nc, nk, wukt, wuvt, q_s, qr_s, o_s, m_s, l_s, bias_s, ob_s, y_v, pc_v, pk_v,
         loc_sem, send_sem, recv_sem):
    me = lax.axis_index("pool")
    core = lax.rem(me, 2)
    cx = lax.rem(lax.div(me, 2), 2)
    cy = lax.div(me, 4)
    fp = 1 - 2 * core
    fx = 2 - 4 * cx
    fy = 4 - 8 * cy
    peer = {"p": me + fp, "x": me + fx, "y": me + fy}

    n_loc = [0]

    def local(src, dst):
        cp = pltpu.make_async_copy(src, dst, loc_sem.at[n_loc[0]])
        n_loc[0] += 1
        cp.start()
        return cp

    ld_kr = local(ckr_hbm, ckr_v)
    ld_c = [local(cc_hbm.at[p], kc.at[0, p % 2, p // 2]) for p in range(4)]
    ld_x = local(x_hbm, x_v)
    ld_dkv = local(wdkv_hbm, wdkv_v)
    ld_small = [local(plen_hbm, plen_s), local(tbl_hbm, tbl_v), local(wt_hbm, wt_s), local(g_hbm, g_v)]
    ld_uk = local(wuk_hbm, wuk_v)
    ld_q = [local(wq_hbm.at[:, pl.ds(g * GCOLS, GCOLS)], wq_v.at[g]) for g in range(NGROUP)]
    ld_uv = local(wuv_hbm, wuv_v)
    ld_o = local(wo_hbm, wo_v)

    barrier = pltpu.get_barrier_semaphore()
    for d in ("p", "x", "y"):
        pl.semaphore_signal(barrier, inc=1, device_id=(peer[d],), device_id_type=MESH)

    lane = lax.broadcasted_iota(jnp.int32, (TOK, 128), 1)
    low = lane < RD

    ld_kr.wait()
    for h in range(2):
        krp[0, h] = jnp.concatenate([ckr_v[2 * h], ckr_v[2 * h + 1]], axis=-1)

    def page_copies(name):
        sc, sh, tc, th, d = FLOWS[name]
        i = 2 * FLOW_ID[name]
        return [
            pltpu.make_async_remote_copy(src_ref=kc.at[sc, :, sh], dst_ref=kc.at[tc, :, th], send_sem=send_sem.at[i],
                                         recv_sem=recv_sem.at[i], device_id=(peer[d],), device_id_type=MESH),
            pltpu.make_async_remote_copy(src_ref=krp.at[sc, sh], dst_ref=krp.at[tc, th], send_sem=send_sem.at[i + 1],
                                         recv_sem=recv_sem.at[i + 1], device_id=(peer[d],), device_id_type=MESH),
        ]

    def new_copies(name):
        s, t, d, halves, tag = NEWS[name]
        rows = slice(halves[0], halves[-1] + 1)
        i = NEW_ID[(name, "c")]
        out = [pltpu.make_async_remote_copy(src_ref=nc.at[s, rows], dst_ref=nc.at[t, rows], send_sem=send_sem.at[i],
                                            recv_sem=recv_sem.at[i], device_id=(peer[d],), device_id_type=MESH)]
        if tag:
            i = NEW_ID[(name, "k")]
            out.append(pltpu.make_async_remote_copy(src_ref=nk.at[s], dst_ref=nk.at[t], send_sem=send_sem.at[i],
                                                    recv_sem=recv_sem.at[i], device_id=(peer[d],), device_id_type=MESH))
        return out

    started = []

    def send(name):
        for cp in (page_copies if name in FLOWS else new_copies)(name):
            cp.start()
            started.append(cp)

    def arrived(name):
        for cp in (page_copies if name in FLOWS else new_copies)(name):
            cp.wait_recv()

    pl.semaphore_wait(barrier, 3)
    for cp in ld_c:
        cp.wait()
    for name in ("x0", "y1", "p0", "p1", "x1", "y0"):
        send(name)

    out_cps = [local(kc.at[0, p % 2, p // 2], cco_hbm.at[p]) for p in range(4)]
    out_cps.append(local(ckr_v.at[pl.ds(0, 4)], ckro_hbm.at[pl.ds(0, 4)]))

    for cp in ld_small:
        cp.wait()
    k_lane = lax.rem(lane, 32)
    freq = jnp.zeros((TOK, 128), F32)
    for k, f in enumerate(INV_FREQ):
        freq = jnp.where(k_lane == k, f, freq)
    pos = (lax.broadcasted_iota(jnp.int32, (TOK, 128), 0) + plen_s[0]).astype(F32)
    ang = pos * freq
    cos_t = jnp.cos(ang)
    sin_t = jnp.sin(ang)
    sin_t = jnp.where(lax.rem(lane, 64) < 32, -sin_t, sin_t)

    def rope2(v64):
        v = jnp.concatenate([v64, v64], axis=-1)
        return v * cos_t + pltpu.roll(v, 32, 1) * sin_t

    ld_x.wait()
    ld_dkv.wait()
    kv = lax.dot_general(x_v[...], wdkv_v[...], (((1,), (1,)), ((), ())), preferred_element_type=F32)
    latp = kv[:, :LAT]
    inv_rms = lax.rsqrt(jnp.mean(latp * latp, axis=-1, keepdims=True) + EPS)
    c_new = (latp * inv_rms * g_v[...].astype(F32)).astype(BF)
    kr_dup = rope2(kv[:, LAT:]).astype(BF)
    nc[0, 0] = c_new[:32]
    nc[0, 1] = c_new[32:]
    nk[0, pl.ds(0, 32)] = jnp.where(low[:32], kr_dup[:32], kr_dup[32:])
    nk[0, pl.ds(32, 16)] = jnp.full((16, 128), wt_s[0, 0], jnp.int32).astype(F32).astype(BF)

    tbl = tbl_v[...]
    ids = (tbl[0:1] * 4 + tbl[1:2]).astype(F32)
    ids_col = jnp.transpose(jnp.broadcast_to(ids, (128, 256)))
    seg = lax.div(lax.broadcasted_iota(jnp.int32, (1, 256), 1), 64)
    flips = {0: 0, 1: fp, 2: fx, 4: fy, 3: fp + fx, 5: fp + fy, 6: fx + fy, 7: fp + fx + fy}
    for c, ((ra, ha), (rb, hb)) in enumerate(CHUNKS):
        pa = (me + flips[ra]) * 4 + 2 * ha
        pb = (me + flips[rb]) * 4 + 2 * hb
        want = jnp.where(seg == 0, pa, jnp.where(seg == 1, pb, jnp.where(seg == 2, pa + 1, pb + 1))).astype(F32)
        parts = []
        for t in range(2):
            hit = jnp.where(ids_col == want[:, t * 128:(t + 1) * 128], 1.0, 0.0)
            parts.append(jnp.sum(hit, axis=0, keepdims=True))
        cnt = jnp.concatenate(parts, axis=-1)
        bias_s[c] = jnp.where(cnt > 0.0, jnp.log2(jnp.maximum(cnt, 1.0)), -jnp.inf)

    r_i = lax.broadcasted_iota(jnp.int32, (256, 256), 0)
    c_i = lax.broadcasted_iota(jnp.int32, (256, 256), 1)
    perm = (r_i == lax.rem(c_i, 16) * 16 + lax.div(c_i, 16)).astype(F32).astype(BF)

    def reorder(src, dst):
        def step(b, carry):
            for u in range(4):
                blk = b * 4 + u
                rows = src[pl.ds(pl.multiple_of(blk * 256, 256), 256), :]
                t = jnp.dot(perm, rows, preferred_element_type=F32).astype(BF)
                dst[:, pl.ds(pl.multiple_of(blk * 16, 16), 16), :] = t.reshape(NH, 16, 128)
            return carry
        lax.fori_loop(0, 8, step, 0)

    ld_uk.wait()
    reorder(wuk_v, wukt)

    for g in range(NGROUP):
        ld_q[g].wait()
        qg = jnp.dot(x_v[...], wq_v[g], preferred_element_type=F32).astype(BF).astype(F32)
        for k in range(GROUP):
            h = g * GROUP + k
            nope = qg[:, k * HQ:k * HQ + ND].astype(BF)
            qr_s[pl.ds(h * TOK, TOK), :] = rope2(qg[:, k * HQ + ND:(k + 1) * HQ]).astype(BF)
            q_s[pl.ds(h * TOK, TOK), :] = lax.dot_general(
                nope, wukt[h], (((1,), (1,)), ((), ())), preferred_element_type=F32).astype(BF)

    NT = (((1,), (1,)), ((), ()))
    kr_low = jnp.where(low, kr_dup.astype(F32), 0.0).astype(BF)
    row_tok = lax.rem(lax.broadcasted_iota(jnp.int32, (BLK, TOK), 0), TOK)
    key_tok = lax.broadcasted_iota(jnp.int32, (BLK, TOK), 1)
    causal = key_tok <= row_tok
    for b in range(ROWS // BLK):
        rows = pl.ds(b * BLK, BLK)
        s = lax.dot_general(q_s[rows, :], c_new, NT, preferred_element_type=F32)
        s = s + lax.dot_general(qr_s[rows, :], kr_low, NT, preferred_element_type=F32)
        t = jnp.where(causal, s * SCALE2, -jnp.inf)
        mx = jnp.max(t, axis=-1, keepdims=True)
        p = jnp.exp2(t - mx)
        m_s[rows, :] = jnp.broadcast_to(mx, (BLK, 128))
        l_s[rows, :] = jnp.concatenate([p, jnp.zeros_like(p)], axis=-1)
        o_s[rows, :] = jnp.dot(p.astype(BF), c_new, preferred_element_type=F32)

    lane2 = lax.broadcasted_iota(jnp.int32, (128, 128), 1)

    def attend(c):
        keys = kc[c].reshape(256, LAT)
        kp = krp[c].reshape(128, 128).astype(F32)
        kbd = jnp.concatenate([jnp.where(lane2 < RD, kp, 0.0), jnp.where(lane2 < RD, 0.0, kp)], axis=0).astype(BF)
        bias = bias_s[c]
        for b in range(ROWS // BLK):
            rows = pl.ds(b * BLK, BLK)
            s = lax.dot_general(q_s[rows, :], keys, NT, preferred_element_type=F32)
            s = s + lax.dot_general(qr_s[rows, :], kbd, NT, preferred_element_type=F32)
            t = s * SCALE2 + bias
            mx = jnp.max(jnp.maximum(t[:, :128], t[:, 128:]), axis=-1, keepdims=True)
            m_old = m_s[rows, :]
            m_new = jnp.maximum(m_old, jnp.broadcast_to(mx, (BLK, 128)))
            alpha = jnp.exp2(m_old - m_new)
            p = jnp.exp2(t - jnp.concatenate([m_new, m_new], axis=-1))
            m_s[rows, :] = m_new
            l_s[rows, :] = l_s[rows, :] * alpha + (p[:, :128] + p[:, 128:])
            a4 = jnp.concatenate([alpha] * 4, axis=-1)
            o_s[rows, :] = o_s[rows, :] * a4 + jnp.dot(p.astype(BF), keys, preferred_element_type=F32)

    for name in ("x0", "y1"):
        arrived(name)
    for name in ("dy", "dx", "p20", "p21"):
        send(name)
    for name in ("nx", "ny", "np"):
        send(name)
    attend(0)
    for name in ("p0", "p1"):
        arrived(name)
    attend(1)
    attend(2)
    ld_uv.wait()
    reorder(wuv_v, wuvt)
    for name in ("x1", "y0"):
        arrived(name)
    for name in ("p40", "p41"):
        send(name)
    attend(4)
    for name in ("p20", "p21"):
        arrived(name)
    attend(3)
    for name in ("p40", "p41"):
        arrived(name)
    attend(5)
    for name in ("dy", "dx"):
        arrived(name)
    for name in ("p60", "p61"):
        send(name)
    for name in ("nx", "ny"):
        arrived(name)
    for name in ("ndy", "ndx", "n2p", "n4p"):
        send(name)
    attend(6)
    for name in ("p60", "p61"):
        arrived(name)
    attend(7)

    for h in range(NH):
        rows = pl.ds(h * TOK, TOK)
        denom = jnp.sum(l_s[rows, :], axis=-1, keepdims=True)
        ol = (o_s[rows, :] / denom).astype(BF)
        ob_s[:, pl.ds(h * ND, ND)] = jnp.dot(ol, wuvt[h], preferred_element_type=F32).astype(BF)
    for name in ("ndy", "ndx"):
        arrived(name)
    send("n6p")
    ld_o.wait()
    NB = 512

    def out_step(j, carry):
        cols = pl.ds(pl.multiple_of(j * NB, NB), NB)
        acc = jnp.dot(ob_s[...], wo_v[:, cols], preferred_element_type=F32)
        y_v[:, cols] = (x_v[:, cols].astype(F32) + acc).astype(BF)
        return carry
    lax.fori_loop(0, DM // NB, out_step, 0)
    y_cp = local(y_v, y_hbm)

    for name in ("np", "n2p", "n4p", "n6p"):
        arrived(name)
    mine = me.astype(F32)
    pc = [jnp.zeros((32, LAT), F32) for _ in range(2)]
    pk = jnp.zeros((32, 128), F32)
    for r in range(8):
        hit = nk[r, pl.ds(32, 16)].astype(F32)
        hit = jnp.concatenate([hit, hit], axis=0) == mine
        pk = jnp.where(hit, nk[r, pl.ds(0, 32)].astype(F32), pk)
        hit4 = jnp.concatenate([hit] * 4, axis=-1)
        for u in range(2):
            pc[u] = jnp.where(hit4, nc[r, u].astype(F32), pc[u])
    pc_v[pl.ds(0, 32), :] = pc[0].astype(BF)
    pc_v[pl.ds(32, 32), :] = pc[1].astype(BF)
    pkb = pk.astype(BF)
    pk_v[pl.ds(0, 32), :] = pkb[:, :RD]
    pk_v[pl.ds(32, 32), :] = pkb[:, RD:]
    out_cps.append(local(pc_v, cco_hbm.at[4]))
    out_cps.append(local(pk_v, ckro_hbm.at[4]))
    for cp in started:
        cp.wait_send()
    y_cp.wait()
    for cp in out_cps:
        cp.wait()


def fused(x, plen, tbl, wt, cc, ckr, wq, wdkv, g, wuk, wuv, wo):
    any_spec = pl.BlockSpec(memory_space=pl.ANY)
    dma = pltpu.SemaphoreType.DMA
    return pl.pallas_call(
        body,
        name="mla_prefill",
        out_shape=(
            jax.ShapeDtypeStruct((TOK, DM), BF),
            jax.ShapeDtypeStruct((5, TOK, LAT), BF),
            jax.ShapeDtypeStruct((5, TOK, RD), BF),
        ),
        in_specs=[any_spec] * 12,
        out_specs=(any_spec,) * 3,
        scratch_shapes=[
            pltpu.VMEM((TOK, DM), BF),
            pltpu.SMEM((1,), jnp.int32),
            pltpu.VMEM((2, 256), jnp.int32),
            pltpu.SMEM((1, 2), jnp.int32),
            pltpu.VMEM((5, TOK, RD), BF),
            pltpu.VMEM((NGROUP, DM, GCOLS), BF),
            pltpu.VMEM((LAT + RD, DM), BF),
            pltpu.VMEM((1, LAT), BF),
            pltpu.VMEM((LAT * NH, ND), BF),
            pltpu.VMEM((LAT * NH, ND), BF),
            pltpu.VMEM((DM, DM), BF),
            pltpu.VMEM((8, 2, 2, TOK, LAT), BF),
            pltpu.VMEM((8, 2, TOK, 128), BF),
            pltpu.VMEM((8, 2, 32, LAT), BF),
            pltpu.VMEM((8, 48, 128), BF),
            pltpu.VMEM((NH, LAT, ND), BF),
            pltpu.VMEM((NH, LAT, ND), BF),
            pltpu.VMEM((ROWS, LAT), BF),
            pltpu.VMEM((ROWS, 128), BF),
            pltpu.VMEM((ROWS, LAT), F32),
            pltpu.VMEM((ROWS, 128), F32),
            pltpu.VMEM((ROWS, 128), F32),
            pltpu.VMEM((8, 1, 256), F32),
            pltpu.VMEM((TOK, DM), BF),
            pltpu.VMEM((TOK, DM), BF),
            pltpu.VMEM((TOK, LAT), BF),
            pltpu.VMEM((TOK, RD), BF),
            dma((32,)),
            dma((NSEM,)),
            dma((NSEM,)),
        ],
        compiler_params=pltpu.CompilerParams(collective_id=0, has_side_effects=True, vmem_limit_bytes=60 * 1024 * 1024),
    )(x, plen, tbl, wt, cc, ckr, wq, wdkv, g, wuk, wuv, wo)


def solution(mesh):
    def device_step(hidden, pre_len, pre_table, wr_table, cache_c, cache_kr, w_q, w_dkv, g_kv, w_uk, w_uv, w_o):
        y, c_out, kr_out = fused(
            hidden.reshape(TOK, DM), pre_len, pre_table.reshape(256, 2).T, wr_table.reshape(1, 2), cache_c[0], cache_kr[0],
            w_q, w_dkv.T, g_kv.reshape(1, LAT), w_uk.reshape(LAT * NH, ND), w_uv.reshape(LAT * NH, ND), w_o)
        return y[None], c_out[None], kr_out[None]

    row = P("pool")
    rep = P()
    return jax.shard_map(device_step, mesh=mesh, in_specs=(row,) * 6 + (rep,) * 6, out_specs=(row, row, row), check_vma=False)
```

```python
import contextlib
import math

import jax
import jax.numpy as jnp
import numpy as np
from jax import lax
from jax.experimental import pallas as pl
from jax.experimental.pallas import tpu as pltpu
from jax.sharding import PartitionSpec as P

BF = jnp.bfloat16
PROF = False
F32 = jnp.float32
MESH = pl.DeviceIdType.MESH

TOK = 64
DM = 2048
NH = 16
LAT = 512
RD = 64
ND = 128
HQ = ND + RD
ROWS = NH * TOK
EPS = 1e-6
GROUP = 4
GCOLS = GROUP * HQ
NGROUP = NH // GROUP
BLK = 256
SCALE2 = float((ND + RD) ** -0.5 * math.log2(math.e))
INV_FREQ = [float(np.float32(10000.0 ** (-k / 32.0))) for k in range(32)]

CHUNKS = (
    ((0, 0), (0, 1)),
    ((1, 0), (1, 1)),
    ((2, 0), (4, 1)),
    ((3, 0), (5, 1)),
    ((2, 1), (4, 0)),
    ((3, 1), (5, 0)),
    ((6, 0), (6, 1)),
    ((7, 0), (7, 1)),
)

FLOWS = {
    "x0": (0, 0, 2, 0, "x"),
    "x1": (0, 1, 4, 0, "x"),
    "y1": (0, 1, 2, 1, "y"),
    "y0": (0, 0, 4, 1, "y"),
    "p0": (0, 0, 1, 0, "p"),
    "p1": (0, 1, 1, 1, "p"),
    "dy": (2, 0, 6, 0, "y"),
    "dx": (2, 1, 6, 1, "x"),
    "p20": (2, 0, 3, 0, "p"),
    "p21": (2, 1, 3, 1, "p"),
    "p40": (4, 0, 5, 0, "p"),
    "p41": (4, 1, 5, 1, "p"),
    "p60": (6, 0, 7, 0, "p"),
    "p61": (6, 1, 7, 1, "p"),
}
FLOW_ID = {name: i for i, name in enumerate(FLOWS)}
NF = 2 * len(FLOWS)

NEWS = {
    "nx": (0, 2, "x", (0, 1), True),
    "ny": (0, 4, "y", (0, 1), True),
    "np": (0, 1, "p", (0, 1), True),
    "n2p": (2, 3, "p", (0, 1), True),
    "n4p": (4, 5, "p", (0, 1), True),
    "ndy": (2, 6, "y", (0,), False),
    "ndx": (4, 6, "x", (1,), True),
    "n6p": (6, 7, "p", (0, 1), True),
}
NEW_ID = {}
for _name, (_s, _t, _d, _h, _k) in NEWS.items():
    for _part in ("c", "k"):
        if _part == "c" or _k:
            NEW_ID[(_name, _part)] = NF + len(NEW_ID)
NSEM = NF + len(NEW_ID)


def scope(name):
    return jax.named_scope(name) if PROF else contextlib.nullcontext()


def body(x_hbm, plen_hbm, tbl_hbm, wt_hbm, cc_hbm, ckr_hbm, wq_hbm, wdkv_hbm, g_hbm, wuk_hbm, wuv_hbm, wo_hbm,
         y_hbm, cco_hbm, ckro_hbm,
         x_v, plen_s, tbl_v, wt_s, ckr_v, wq_v, wdkv_v, g_v, wuk_v, wuv_v, wo_v,
         kc, krp, nc, nk, wukt, wuvt, q_s, qr_s, s_s, o_s, m_s, l_s, bias_s, ob_s, y_v, pc_v, pk_v,
         loc_sem, send_sem, recv_sem):
    me = lax.axis_index("pool")
    core = lax.rem(me, 2)
    cx = lax.rem(lax.div(me, 2), 2)
    cy = lax.div(me, 4)
    fp = 1 - 2 * core
    fx = 2 - 4 * cx
    fy = 4 - 8 * cy
    peer = {"p": me + fp, "x": me + fx, "y": me + fy}

    barrier = pltpu.get_barrier_semaphore()
    for d in ("p", "x", "y"):
        pl.semaphore_signal(barrier, inc=1, device_id=(peer[d],), device_id_type=MESH)

    n_loc = [0]

    def local(src, dst):
        cp = pltpu.make_async_copy(src, dst, loc_sem.at[n_loc[0]])
        n_loc[0] += 1
        cp.start()
        return cp

    ld_kr = local(ckr_hbm, ckr_v)
    ld_c = [local(cc_hbm.at[p], kc.at[0, p % 2, p // 2]) for p in range(4)]
    ld_x = local(x_hbm, x_v)
    ld_dkv = local(wdkv_hbm, wdkv_v)
    ld_small = [local(plen_hbm, plen_s), local(tbl_hbm, tbl_v), local(wt_hbm, wt_s), local(g_hbm, g_v)]
    ld_uk = local(wuk_hbm, wuk_v)
    ld_q = [local(wq_hbm.at[:, pl.ds(g * GCOLS, GCOLS)], wq_v.at[g]) for g in range(NGROUP)]
    ld_uv = local(wuv_hbm, wuv_v)
    ld_o = local(wo_hbm, wo_v)


    lane = lax.broadcasted_iota(jnp.int32, (TOK, 128), 1)
    low = lane < RD

    ld_kr.wait()
    for h in range(2):
        krp[0, h] = jnp.concatenate([ckr_v[2 * h], ckr_v[2 * h + 1]], axis=-1)

    def page_copies(name):
        sc, sh, tc, th, d = FLOWS[name]
        i = 2 * FLOW_ID[name]
        return [
            pltpu.make_async_remote_copy(src_ref=kc.at[sc, :, sh], dst_ref=kc.at[tc, :, th], send_sem=send_sem.at[i],
                                         recv_sem=recv_sem.at[i], device_id=(peer[d],), device_id_type=MESH),
            pltpu.make_async_remote_copy(src_ref=krp.at[sc, sh], dst_ref=krp.at[tc, th], send_sem=send_sem.at[i + 1],
                                         recv_sem=recv_sem.at[i + 1], device_id=(peer[d],), device_id_type=MESH),
        ]

    def new_copies(name):
        s, t, d, halves, tag = NEWS[name]
        rows = slice(halves[0], halves[-1] + 1)
        i = NEW_ID[(name, "c")]
        out = [pltpu.make_async_remote_copy(src_ref=nc.at[s, rows], dst_ref=nc.at[t, rows], send_sem=send_sem.at[i],
                                            recv_sem=recv_sem.at[i], device_id=(peer[d],), device_id_type=MESH)]
        if tag:
            i = NEW_ID[(name, "k")]
            out.append(pltpu.make_async_remote_copy(src_ref=nk.at[s], dst_ref=nk.at[t], send_sem=send_sem.at[i],
                                                    recv_sem=recv_sem.at[i], device_id=(peer[d],), device_id_type=MESH))
        return out

    started = []

    def send(name):
        for cp in (page_copies if name in FLOWS else new_copies)(name):
            cp.start()
            started.append(cp)

    def arrived(name):
        for cp in (page_copies if name in FLOWS else new_copies)(name):
            cp.wait_recv()

    with scope("barrier_send"):
        pl.semaphore_wait(barrier, 3)
        for cp in ld_c:
            cp.wait()
        for name in ("x0", "y1", "p0", "p1", "x1", "y0"):
            send(name)

    out_cps = [local(kc.at[0, p % 2, p // 2], cco_hbm.at[p]) for p in range(4)]
    out_cps.append(local(ckr_v.at[pl.ds(0, 4)], ckro_hbm.at[pl.ds(0, 4)]))

    with scope("tables"):
        for cp in ld_small:
            cp.wait()
        k_lane = lax.rem(lane, 32)
        freq = jnp.zeros((TOK, 128), F32)
        for k, f in enumerate(INV_FREQ):
            freq = jnp.where(k_lane == k, f, freq)
        pos = (lax.broadcasted_iota(jnp.int32, (TOK, 128), 0) + plen_s[0]).astype(F32)
        ang = pos * freq
        cos_t = jnp.cos(ang)
        sin_t = jnp.sin(ang)
        sin_t = jnp.where(lax.rem(lane, 64) < 32, -sin_t, sin_t)

    def rope2(v64):
        v = jnp.concatenate([v64, v64], axis=-1)
        return v * cos_t + pltpu.roll(v, 32, 1) * sin_t

    with scope("newlat"):
        ld_x.wait()
        ld_dkv.wait()
        kv = lax.dot_general(x_v[...], wdkv_v[...], (((1,), (1,)), ((), ())), preferred_element_type=F32)
        latp = kv[:, :LAT]
        inv_rms = lax.rsqrt(jnp.mean(latp * latp, axis=-1, keepdims=True) + EPS)
        c_new = (latp * inv_rms * g_v[...].astype(F32).reshape(1, LAT)).astype(BF)
        kr_dup = rope2(kv[:, LAT:]).astype(BF)
        nc[0, 0] = c_new[:32]
        nc[0, 1] = c_new[32:]
        nk[0, pl.ds(0, 32)] = jnp.where(low[:32], kr_dup[:32], kr_dup[32:])
        nk[0, pl.ds(32, 16)] = jnp.full((16, 128), wt_s[0, 0], jnp.int32).astype(F32).astype(BF)

    with scope("mult"):
        tbl = tbl_v[...]
        ids = (tbl[0:1] * 4 + tbl[1:2]).astype(F32)
        ids_col = jnp.transpose(jnp.broadcast_to(ids, (128, 256)))
        seg = lax.div(lax.broadcasted_iota(jnp.int32, (1, 256), 1), 64)
        flips = {0: 0, 1: fp, 2: fx, 4: fy, 3: fp + fx, 5: fp + fy, 6: fx + fy, 7: fp + fx + fy}
        for c, ((ra, ha), (rb, hb)) in enumerate(CHUNKS):
            pa = (me + flips[ra]) * 4 + 2 * ha
            pb = (me + flips[rb]) * 4 + 2 * hb
            want = jnp.where(seg == 0, pa, jnp.where(seg == 1, pb, jnp.where(seg == 2, pa + 1, pb + 1))).astype(F32)
            parts = []
            for t in range(2):
                hit = jnp.where(ids_col == want[:, t * 128:(t + 1) * 128], 1.0, 0.0)
                parts.append(jnp.sum(hit, axis=0, keepdims=True))
            cnt = jnp.concatenate(parts, axis=-1)
            bias_s[c] = jnp.where(cnt > 0.0, jnp.log2(jnp.maximum(cnt, 1.0)), -jnp.inf)

    r_i = lax.broadcasted_iota(jnp.int32, (256, 256), 0)
    c_i = lax.broadcasted_iota(jnp.int32, (256, 256), 1)
    perm = (r_i == lax.rem(c_i, 16) * 16 + lax.div(c_i, 16)).astype(F32).astype(BF)

    def reorder(src, dst):
        def step(i, carry):
            for u in range(4):
                blk = i * 8 + 2 * u
                rows = [src[pl.ds(pl.multiple_of((blk + v) * 256, 256), 256), :] for v in range(2)]
                t = jnp.dot(perm, jnp.concatenate(rows, axis=-1), preferred_element_type=F32).astype(BF)
                for v in range(2):
                    dst[:, pl.ds(pl.multiple_of((blk + v) * 16, 16), 16), :] = t[:, v * 128:(v + 1) * 128].reshape(NH, 16, 128)
            return carry
        lax.fori_loop(0, 4, step, 0)

    with scope("reorder_uk"):
        ld_uk.wait()
        reorder(wuk_v, wukt)

    for g in range(NGROUP):
        with scope(f"waitq{g}"):
            ld_q[g].wait()
        with scope(f"query{g}"):
            qg = jnp.dot(x_v[...], wq_v[g], preferred_element_type=F32).astype(BF).astype(F32)
            for k in range(GROUP):
                h = g * GROUP + k
                nope = qg[:, k * HQ:k * HQ + ND].astype(BF)
                qr_s[pl.ds(h * TOK, TOK), :] = rope2(qg[:, k * HQ + ND:(k + 1) * HQ]).astype(BF)
                q_s[pl.ds(h * TOK, TOK), :] = lax.dot_general(
                    nope, wukt[h], (((1,), (1,)), ((), ())), preferred_element_type=F32).astype(BF)

    NT = (((1,), (1,)), ((), ()))
    row_tok = lax.rem(lax.broadcasted_iota(jnp.int32, (BLK, TOK), 0), TOK)
    causal = lax.broadcasted_iota(jnp.int32, (BLK, TOK), 1) <= row_tok
    lane2 = lax.broadcasted_iota(jnp.int32, (128, 128), 1)
    kr_low = jnp.where(low, kr_dup.astype(F32), 0.0).astype(BF)

    def rope_keys(c):
        if c < 0:
            return kr_low
        kp = krp[c].reshape(128, 128).astype(F32)
        return jnp.concatenate([jnp.where(lane2 < RD, kp, 0.0), jnp.where(lane2 < RD, 0.0, kp)], axis=0).astype(BF)

    def keys_of(c):
        return nc[0].reshape(TOK, LAT) if c < 0 else kc[c].reshape(256, LAT)

    def scores(c, b, slot, kbd):
        rows = pl.ds(b * BLK, BLK)
        s = lax.dot_general(q_s[rows, :], keys_of(c), NT, preferred_element_type=F32)
        s = s + lax.dot_general(qr_s[rows, :], kbd, NT, preferred_element_type=F32)
        if c < 0:
            s_s[slot, :, :TOK] = s
        else:
            s_s[slot] = s

    def accumulate(c, b, slot):
        rows = pl.ds(b * BLK, BLK)
        if c < 0:
            t = jnp.where(causal, s_s[slot, :, :TOK] * SCALE2, -jnp.inf)
            mx = jnp.max(t, axis=-1, keepdims=True)
            p = jnp.exp2(t - mx)
            m_s[rows, :] = jnp.broadcast_to(mx, (BLK, 128))
            l_s[rows, :] = jnp.concatenate([p, jnp.zeros_like(p)], axis=-1)
            o_s[rows, :] = jnp.dot(p.astype(BF), keys_of(c), preferred_element_type=F32)
            return
        bias = bias_s[c]
        t = s_s[slot] * SCALE2 + bias
        mx = jnp.max(jnp.maximum(t[:, :128], t[:, 128:]), axis=-1, keepdims=True)
        m_old = m_s[rows, :]
        m_new = jnp.maximum(m_old, jnp.broadcast_to(mx, (BLK, 128)))
        alpha = jnp.exp2(m_old - m_new)
        p = jnp.exp2(t - jnp.concatenate([m_new, m_new], axis=-1))
        m_s[rows, :] = m_new
        l_s[rows, :] = l_s[rows, :] * alpha + (p[:, :128] + p[:, 128:])
        a4 = jnp.concatenate([alpha] * 4, axis=-1)
        o_s[rows, :] = o_s[rows, :] * a4 + jnp.dot(p.astype(BF), keys_of(c), preferred_element_type=F32)

    def arrive(*names):
        with scope("wait_" + names[0]):
            for name in names:
                arrived(name)

    def sends(*names):
        for name in names:
            send(name)

    def before(c):
        if c == 0:
            arrive("x0", "y1")
            sends("dy", "dx", "p20", "p21", "nx", "ny", "np")
        elif c == 1:
            arrive("p0", "p1")
        elif c == 3:
            arrive("p20", "p21")
        elif c == 4:
            arrive("x1", "y0")
            sends("p40", "p41")
        elif c == 5:
            arrive("p40", "p41")
        elif c == 6:
            arrive("dy", "dx")
            sends("p60", "p61")
            arrive("nx", "ny")
            sends("ndy", "ndx", "n2p", "n4p")
        elif c == 7:
            arrive("p60", "p61")

    nblk = ROWS // BLK
    prev = None
    for c in (-1, 0, 1, 2, 4, 3, 5, 6, 7):
        before(c)
        if c == 4:
            with scope("reorder_uv"):
                ld_uv.wait()
                reorder(wuv_v, wuvt)
        with scope(f"attend{c}"):
            kbd = rope_keys(c)
            for b in range(nblk):
                scores(c, b, b % 2, kbd)
                if prev is not None:
                    accumulate(*prev)
                prev = (c, b, b % 2)
    with scope("attend_last"):
        accumulate(*prev)

    with scope("values"):
        for h in range(NH):
            rows = pl.ds(h * TOK, TOK)
            denom = jnp.sum(l_s[rows, :], axis=-1, keepdims=True)
            ol = (o_s[rows, :] / denom).astype(BF)
            ob_s[:, pl.ds(h * ND, ND)] = jnp.dot(ol, wuvt[h], preferred_element_type=F32).astype(BF)
    with scope("wait_ndy"):
        for name in ("ndy", "ndx"):
            arrived(name)
    send("n6p")
    with scope("wait_wo"):
        ld_o.wait()
    NB = 512

    def out_step(j, carry):
        cols = pl.ds(pl.multiple_of(j * NB, NB), NB)
        acc = jnp.dot(ob_s[...], wo_v[:, cols], preferred_element_type=F32)
        y_v[:, cols] = (x_v[:, cols].astype(F32) + acc).astype(BF)
        return carry
    with scope("outproj"):
        lax.fori_loop(0, DM // NB, out_step, 0)
    y_cp = local(y_v, y_hbm)

    with scope("wait_np"):
        for name in ("np", "n2p", "n4p", "n6p"):
            arrived(name)
    with scope("page"):
        mine = me.astype(F32)
        pc = [jnp.zeros((32, LAT), F32) for _ in range(2)]
        pk = jnp.zeros((32, 128), F32)
        for r in range(8):
            hit = nk[r, pl.ds(32, 16)].astype(F32)
            hit = jnp.concatenate([hit, hit], axis=0) == mine
            pk = jnp.where(hit, nk[r, pl.ds(0, 32)].astype(F32), pk)
            hit4 = jnp.concatenate([hit] * 4, axis=-1)
            for u in range(2):
                pc[u] = jnp.where(hit4, nc[r, u].astype(F32), pc[u])
        pc_v[pl.ds(0, 32), :] = pc[0].astype(BF)
        pc_v[pl.ds(32, 32), :] = pc[1].astype(BF)
        pkb = pk.astype(BF)
        pk_v[pl.ds(0, 32), :] = pkb[:, :RD]
        pk_v[pl.ds(32, 32), :] = pkb[:, RD:]
        out_cps.append(local(pc_v, cco_hbm.at[4]))
        out_cps.append(local(pk_v, ckro_hbm.at[4]))
    with scope("final_wait"):
        for cp in started:
            cp.wait_send()
        y_cp.wait()
        for cp in out_cps:
            cp.wait()


def fused(x, plen, tbl, wt, cc, ckr, wq, wdkv, g, wuk, wuv, wo):
    any_spec = pl.BlockSpec(memory_space=pl.ANY)
    dma = pltpu.SemaphoreType.DMA
    return pl.pallas_call(
        body,
        name="mla_prefill",
        out_shape=(
            jax.ShapeDtypeStruct((TOK, DM), BF),
            jax.ShapeDtypeStruct((5, TOK, LAT), BF),
            jax.ShapeDtypeStruct((5, TOK, RD), BF),
        ),
        in_specs=[any_spec] * 12,
        out_specs=(any_spec,) * 3,
        scratch_shapes=[
            pltpu.VMEM((TOK, DM), BF),
            pltpu.SMEM((1,), jnp.int32),
            pltpu.VMEM((2, 256), jnp.int32),
            pltpu.SMEM((1, 2), jnp.int32),
            pltpu.VMEM((5, TOK, RD), BF),
            pltpu.VMEM((NGROUP, DM, GCOLS), BF),
            pltpu.VMEM((LAT + RD, DM), BF),
            pltpu.VMEM((LAT,), BF),
            pltpu.VMEM((LAT * NH, ND), BF),
            pltpu.VMEM((LAT * NH, ND), BF),
            pltpu.VMEM((DM, DM), BF),
            pltpu.VMEM((8, 2, 2, TOK, LAT), BF),
            pltpu.VMEM((8, 2, TOK, 128), BF),
            pltpu.VMEM((8, 2, 32, LAT), BF),
            pltpu.VMEM((8, 48, 128), BF),
            pltpu.VMEM((NH, LAT, ND), BF),
            pltpu.VMEM((NH, LAT, ND), BF),
            pltpu.VMEM((ROWS, LAT), BF),
            pltpu.VMEM((ROWS, 128), BF),
            pltpu.VMEM((2, BLK, 256), F32),
            pltpu.VMEM((ROWS, LAT), F32),
            pltpu.VMEM((ROWS, 128), F32),
            pltpu.VMEM((ROWS, 128), F32),
            pltpu.VMEM((8, 1, 256), F32),
            pltpu.VMEM((TOK, DM), BF),
            pltpu.VMEM((TOK, DM), BF),
            pltpu.VMEM((TOK, LAT), BF),
            pltpu.VMEM((TOK, RD), BF),
            dma((32,)),
            dma((NSEM,)),
            dma((NSEM,)),
        ],
        compiler_params=pltpu.CompilerParams(collective_id=0, has_side_effects=True, vmem_limit_bytes=60 * 1024 * 1024),
    )(x, plen, tbl, wt, cc, ckr, wq, wdkv, g, wuk, wuv, wo)


def solution(mesh):
    def device_step(hidden, pre_len, pre_table, wr_table, cache_c, cache_kr, w_q, w_dkv, g_kv, w_uk, w_uv, w_o):
        y, c_out, kr_out = fused(
            hidden.reshape(TOK, DM), pre_len, pre_table.reshape(256, 2).T, wr_table.reshape(1, 2), cache_c[0], cache_kr[0],
            w_q, w_dkv.T, g_kv, w_uk.reshape(LAT * NH, ND), w_uv.reshape(LAT * NH, ND), w_o)
        return y[None], c_out[None], kr_out[None]

    row = P("pool")
    rep = P()
    return jax.shard_map(device_step, mesh=mesh, in_specs=(row,) * 6 + (rep,) * 6, out_specs=(row, row, row), check_vma=False)
```

```python
import contextlib
import math

import jax
import jax.numpy as jnp
import numpy as np
from jax import lax
from jax.experimental import pallas as pl
from jax.experimental.pallas import tpu as pltpu
from jax.sharding import PartitionSpec as P

BF = jnp.bfloat16
PROF = False
F32 = jnp.float32
MESH = pl.DeviceIdType.MESH

TOK = 64
DM = 2048
NH = 16
LAT = 512
RD = 64
ND = 128
HQ = ND + RD
ROWS = NH * TOK
EPS = 1e-6
GROUP = 4
GCOLS = GROUP * HQ
NGROUP = NH // GROUP
BLK = 256
SCALE2 = float((ND + RD) ** -0.5 * math.log2(math.e))
INV_FREQ = [float(np.float32(10000.0 ** (-k / 32.0))) for k in range(32)]

CHUNKS = (
    ((0, 0), (0, 1)),
    ((1, 0), (1, 1)),
    ((2, 0), (4, 1)),
    ((3, 0), (5, 1)),
    ((2, 1), (4, 0)),
    ((3, 1), (5, 0)),
    ((6, 0), (6, 1)),
    ((7, 0), (7, 1)),
)

FLOWS = {
    "x0": (0, 0, 2, 0, "x"),
    "x1": (0, 1, 4, 0, "x"),
    "y1": (0, 1, 2, 1, "y"),
    "y0": (0, 0, 4, 1, "y"),
    "p0": (0, 0, 1, 0, "p"),
    "p1": (0, 1, 1, 1, "p"),
    "dy": (2, 0, 6, 0, "y"),
    "dx": (2, 1, 6, 1, "x"),
    "p20": (2, 0, 3, 0, "p"),
    "p21": (2, 1, 3, 1, "p"),
    "p40": (4, 0, 5, 0, "p"),
    "p41": (4, 1, 5, 1, "p"),
    "p60": (6, 0, 7, 0, "p"),
    "p61": (6, 1, 7, 1, "p"),
}
FLOW_ID = {name: i for i, name in enumerate(FLOWS)}
NF = 2 * len(FLOWS)

NEWS = {
    "nx": (0, 2, "x", (0, 1), True),
    "ny": (0, 4, "y", (0, 1), True),
    "np": (0, 1, "p", (0, 1), True),
    "n2p": (2, 3, "p", (0, 1), True),
    "n4p": (4, 5, "p", (0, 1), True),
    "ndy": (2, 6, "y", (0,), False),
    "ndx": (4, 6, "x", (1,), True),
    "n6p": (6, 7, "p", (0, 1), True),
}
NEW_ID = {}
for _name, (_s, _t, _d, _h, _k) in NEWS.items():
    for _part in ("c", "k"):
        if _part == "c" or _k:
            NEW_ID[(_name, _part)] = NF + len(NEW_ID)
NSEM = NF + len(NEW_ID)


def scope(name):
    return jax.named_scope(name) if PROF else contextlib.nullcontext()


def body(x_hbm, tbl_hbm, wt_hbm, cc_hbm, ckr_hbm, wq_hbm, wdkv_hbm, g_hbm, wuk_hbm, wuv_hbm,
         ob_hbm, pc_hbm, pk_hbm,
         x_v, tbl_v, wt_s, ckr_v, wq_v, wdkv_v, g_v, wuk_v, wuv_v,
         kc, krp, nc, nk, wukt, wuvt, q_s, qn_s, qr_s, s_s, o_s, m_s, l_s, bias_s, ob_s, pc_v, pk_v,
         loc_sem, send_sem, recv_sem):
    me = lax.axis_index("pool")
    core = lax.rem(me, 2)
    cx = lax.rem(lax.div(me, 2), 2)
    cy = lax.div(me, 4)
    fp = 1 - 2 * core
    fx = 2 - 4 * cx
    fy = 4 - 8 * cy
    peer = {"p": me + fp, "x": me + fx, "y": me + fy}

    barrier = pltpu.get_barrier_semaphore()
    for d in ("p", "x", "y"):
        pl.semaphore_signal(barrier, inc=1, device_id=(peer[d],), device_id_type=MESH)

    n_loc = [0]

    def local(src, dst):
        cp = pltpu.make_async_copy(src, dst, loc_sem.at[n_loc[0]])
        n_loc[0] += 1
        cp.start()
        return cp

    ld_kr = local(ckr_hbm, ckr_v)
    ld_c = [local(cc_hbm.at[p], kc.at[0, p % 2, p // 2]) for p in range(4)]
    ld_x = local(x_hbm, x_v)
    ld_dkv = local(wdkv_hbm, wdkv_v)
    ld_small = [local(tbl_hbm, tbl_v), local(wt_hbm, wt_s), local(g_hbm, g_v)]
    ld_uk = local(wuk_hbm, wuk_v)
    ld_q = [local(wq_hbm.at[:, pl.ds(g * GCOLS, GCOLS)], wq_v.at[g]) for g in range(NGROUP)]
    ld_uv = local(wuv_hbm, wuv_v)


    lane = lax.broadcasted_iota(jnp.int32, (TOK, 128), 1)
    low = lane < RD

    ld_kr.wait()
    for h in range(2):
        krp[0, h] = jnp.concatenate([ckr_v[2 * h], ckr_v[2 * h + 1]], axis=-1)

    def page_copies(name):
        sc, sh, tc, th, d = FLOWS[name]
        i = 2 * FLOW_ID[name]
        return [
            pltpu.make_async_remote_copy(src_ref=kc.at[sc, :, sh], dst_ref=kc.at[tc, :, th], send_sem=send_sem.at[i],
                                         recv_sem=recv_sem.at[i], device_id=(peer[d],), device_id_type=MESH),
            pltpu.make_async_remote_copy(src_ref=krp.at[sc, sh], dst_ref=krp.at[tc, th], send_sem=send_sem.at[i + 1],
                                         recv_sem=recv_sem.at[i + 1], device_id=(peer[d],), device_id_type=MESH),
        ]

    def new_copies(name):
        s, t, d, halves, tag = NEWS[name]
        rows = slice(halves[0], halves[-1] + 1)
        i = NEW_ID[(name, "c")]
        out = [pltpu.make_async_remote_copy(src_ref=nc.at[s, rows], dst_ref=nc.at[t, rows], send_sem=send_sem.at[i],
                                            recv_sem=recv_sem.at[i], device_id=(peer[d],), device_id_type=MESH)]
        if tag:
            i = NEW_ID[(name, "k")]
            out.append(pltpu.make_async_remote_copy(src_ref=nk.at[s], dst_ref=nk.at[t], send_sem=send_sem.at[i],
                                                    recv_sem=recv_sem.at[i], device_id=(peer[d],), device_id_type=MESH))
        return out

    started = []

    def send(name):
        for cp in (page_copies if name in FLOWS else new_copies)(name):
            cp.start()
            started.append(cp)

    def arrived(name):
        for cp in (page_copies if name in FLOWS else new_copies)(name):
            cp.wait_recv()

    with scope("barrier"):
        pl.semaphore_wait(barrier, 3)
    with scope("send0"):
        for cp in ld_c:
            cp.wait()
        for name in ("x0", "y1", "p0", "p1", "x1", "y0"):
            send(name)

    with scope("tables"):
        for cp in ld_small:
            cp.wait()
        k_lane = lax.rem(lane, 32)
        freq = jnp.zeros((TOK, 128), F32)
        for k, f in enumerate(INV_FREQ):
            freq = jnp.where(k_lane == k, f, freq)
        n_pages = jnp.sum(jnp.where(tbl_v[0:1] >= 0, 1.0, 0.0), axis=-1, keepdims=True)
        pos = lax.broadcasted_iota(jnp.int32, (TOK, 128), 0).astype(F32) + jnp.broadcast_to(n_pages * TOK, (TOK, 128))
        ang = pos * freq
        cos_t = jnp.cos(ang)
        sin_t = jnp.sin(ang)
        sin_t = jnp.where(lax.rem(lane, 64) < 32, -sin_t, sin_t)

    def rope2(v64):
        v = jnp.concatenate([v64, v64], axis=-1)
        return v * cos_t + pltpu.roll(v, 32, 1) * sin_t

    with scope("newlat"):
        ld_x.wait()
        ld_dkv.wait()
        kv = lax.dot_general(x_v[...], wdkv_v[...], (((1,), (1,)), ((), ())), preferred_element_type=F32)
        latp = kv[:, :LAT]
        inv_rms = lax.rsqrt(jnp.mean(latp * latp, axis=-1, keepdims=True) + EPS)
        c_new = (latp * inv_rms * g_v[...].astype(F32).reshape(1, LAT)).astype(BF)
        kr_dup = rope2(kv[:, LAT:]).astype(BF)
        nc[0, 0] = c_new[:32]
        nc[0, 1] = c_new[32:]
        nk[0, pl.ds(0, 32)] = jnp.where(low[:32], kr_dup[:32], kr_dup[32:])
        nk[0, pl.ds(32, 16)] = jnp.full((16, 128), wt_s[0, 0], jnp.int32).astype(F32).astype(BF)

    with scope("mult"):
        tbl = tbl_v[...]
        ids = (tbl[0:1] * 4 + tbl[1:2]).astype(F32)
        ids_col = jnp.transpose(jnp.broadcast_to(ids, (128, 256)))
        seg = lax.div(lax.broadcasted_iota(jnp.int32, (1, 256), 1), 64)
        flips = {0: 0, 1: fp, 2: fx, 4: fy, 3: fp + fx, 5: fp + fy, 6: fx + fy, 7: fp + fx + fy}
        for c, ((ra, ha), (rb, hb)) in enumerate(CHUNKS):
            pa = (me + flips[ra]) * 4 + 2 * ha
            pb = (me + flips[rb]) * 4 + 2 * hb
            want = jnp.where(seg == 0, pa, jnp.where(seg == 1, pb, jnp.where(seg == 2, pa + 1, pb + 1))).astype(F32)
            parts = []
            for t in range(2):
                hit = jnp.where(ids_col == want[:, t * 128:(t + 1) * 128], 1.0, 0.0)
                parts.append(jnp.sum(hit, axis=0, keepdims=True))
            cnt = jnp.concatenate(parts, axis=-1)
            bias_s[c] = jnp.where(cnt > 0.0, jnp.log2(jnp.maximum(cnt, 1.0)), -jnp.inf)

    r_i = lax.broadcasted_iota(jnp.int32, (256, 256), 0)
    c_i = lax.broadcasted_iota(jnp.int32, (256, 256), 1)
    perm = (r_i == lax.rem(c_i, 16) * 16 + lax.div(c_i, 16)).astype(F32).astype(BF)

    def reorder(src, dst):
        for blk in range(0, 32, 2):
            rows = jnp.concatenate([src[pl.ds((blk + v) * 256, 256), :] for v in range(2)], axis=-1)
            t = jnp.dot(perm, rows, preferred_element_type=F32).astype(BF)
            for v in range(2):
                dst[:, pl.ds((blk + v) * 16, 16), :] = t[:, v * 128:(v + 1) * 128].reshape(NH, 16, 128)

    with scope("reorder_uk"):
        ld_uk.wait()
        reorder(wuk_v, wukt)

    def lift(g):
        for k in range(GROUP):
            h = g * GROUP + k
            q_s[pl.ds(h * TOK, TOK), :] = lax.dot_general(
                qn_s[h], wukt[h], (((1,), (1,)), ((), ())), preferred_element_type=F32).astype(BF)

    for g in range(NGROUP):
        with scope(f"waitq{g}"):
            ld_q[g].wait()
        with scope(f"query{g}"):
            qg = jnp.dot(x_v[...], wq_v[g], preferred_element_type=F32).astype(BF).astype(F32)
            if g:
                lift(g - 1)
            for k in range(GROUP):
                h = g * GROUP + k
                qn_s[h] = qg[:, k * HQ:k * HQ + ND].astype(BF)
                qr_s[pl.ds(h * TOK, TOK), :] = rope2(qg[:, k * HQ + ND:(k + 1) * HQ]).astype(BF)

    NT = (((1,), (1,)), ((), ()))
    row_tok = lax.rem(lax.broadcasted_iota(jnp.int32, (BLK, TOK), 0), TOK)
    causal = lax.broadcasted_iota(jnp.int32, (BLK, TOK), 1) <= row_tok
    lane2 = lax.broadcasted_iota(jnp.int32, (128, 128), 1)
    kr_low = jnp.where(low, kr_dup.astype(F32), 0.0).astype(BF)

    def rope_keys(c):
        if c < 0:
            return kr_low
        kp = krp[c].reshape(128, 128).astype(F32)
        return jnp.concatenate([jnp.where(lane2 < RD, kp, 0.0), jnp.where(lane2 < RD, 0.0, kp)], axis=0).astype(BF)

    def keys_of(c):
        return nc[0].reshape(TOK, LAT) if c < 0 else kc[c].reshape(256, LAT)

    def scores(c, b, slot, kbd):
        rows = pl.ds(b * BLK, BLK)
        s = lax.dot_general(q_s[rows, :], keys_of(c), NT, preferred_element_type=F32)
        s = s + lax.dot_general(qr_s[rows, :], kbd, NT, preferred_element_type=F32)
        if c < 0:
            s_s[slot, :, :TOK] = s
        else:
            s_s[slot] = s

    def accumulate(c, b, slot):
        rows = pl.ds(b * BLK, BLK)
        if c < 0:
            t = jnp.where(causal, s_s[slot, :, :TOK] * SCALE2, -jnp.inf)
            mx = jnp.max(t, axis=-1, keepdims=True)
            p = jnp.exp2(t - mx)
            m_s[rows, :] = jnp.broadcast_to(mx, (BLK, 128))
            l_s[rows, :] = jnp.concatenate([p, jnp.zeros_like(p)], axis=-1)
            o_s[rows, :] = jnp.dot(p.astype(BF), keys_of(c), preferred_element_type=F32)
            return
        bias = bias_s[c]
        t = s_s[slot] * SCALE2 + bias
        mx = jnp.max(jnp.maximum(t[:, :128], t[:, 128:]), axis=-1, keepdims=True)
        m_old = m_s[rows, :]
        m_new = jnp.maximum(m_old, jnp.broadcast_to(mx, (BLK, 128)))
        alpha = jnp.exp2(m_old - m_new)
        p = jnp.exp2(t - jnp.concatenate([m_new, m_new], axis=-1))
        m_s[rows, :] = m_new
        l_s[rows, :] = l_s[rows, :] * alpha + (p[:, :128] + p[:, 128:])
        a4 = jnp.concatenate([alpha] * 4, axis=-1)
        o_s[rows, :] = o_s[rows, :] * a4 + jnp.dot(p.astype(BF), keys_of(c), preferred_element_type=F32)

    def arrive(*names):
        with scope("wait_" + names[0]):
            for name in names:
                arrived(name)

    def sends(*names):
        for name in names:
            send(name)

    def before(c):
        if c == 0:
            arrive("x0", "y1")
            sends("dy", "dx", "p20", "p21", "nx", "ny", "np")
        elif c == 1:
            arrive("p0", "p1")
        elif c == 3:
            arrive("p20", "p21")
        elif c == 4:
            arrive("x1", "y0")
            sends("p40", "p41")
        elif c == 5:
            arrive("p40", "p41")
        elif c == 6:
            arrive("dy", "dx")
            sends("p60", "p61")
            arrive("nx", "ny")
            sends("ndy", "ndx", "n2p", "n4p")
        elif c == 7:
            arrive("p60", "p61")

    nblk = ROWS // BLK
    prev = None
    for c in (-1, 0, 1, 2, 4, 3, 5, 6, 7):
        before(c)
        if c == 4:
            with scope("reorder_uv"):
                ld_uv.wait()
                reorder(wuv_v, wuvt)
        with scope(f"attend{c}"):
            kbd = rope_keys(c)
            for b in range(nblk):
                scores(c, b, b % 2, kbd)
                if prev is None:
                    lift(NGROUP - 1)
                else:
                    accumulate(*prev)
                prev = (c, b, b % 2)
    with scope("attend_last"):
        accumulate(*prev)

    with scope("values"):
        for h in range(NH):
            rows = pl.ds(h * TOK, TOK)
            denom = jnp.sum(l_s[rows, :], axis=-1, keepdims=True)
            ol = (o_s[rows, :] / denom).astype(BF)
            ob_s[:, pl.ds(h * ND, ND)] = jnp.dot(ol, wuvt[h], preferred_element_type=F32).astype(BF)
    arrive("ndy", "ndx")
    send("n6p")
    ob_cp = local(ob_s, ob_hbm)

    arrive("np", "n2p", "n4p", "n6p")
    with scope("page"):
        mine = me.astype(F32)
        pc = [jnp.zeros((32, LAT), F32) for _ in range(2)]
        pk = jnp.zeros((32, 128), F32)
        for r in range(8):
            hit = nk[r, pl.ds(32, 16)].astype(F32)
            hit = jnp.concatenate([hit, hit], axis=0) == mine
            pk = jnp.where(hit, nk[r, pl.ds(0, 32)].astype(F32), pk)
            hit4 = jnp.concatenate([hit] * 4, axis=-1)
            for u in range(2):
                pc[u] = jnp.where(hit4, nc[r, u].astype(F32), pc[u])
        pc_v[pl.ds(0, 32), :] = pc[0].astype(BF)
        pc_v[pl.ds(32, 32), :] = pc[1].astype(BF)
        pkb = pk.astype(BF)
        pk_v[pl.ds(0, 32), :] = pkb[:, :RD]
        pk_v[pl.ds(32, 32), :] = pkb[:, RD:]
        pc_cp = local(pc_v, pc_hbm)
        pk_cp = local(pk_v, pk_hbm)
    with scope("final_wait"):
        for cp in started:
            cp.wait_send()
        ob_cp.wait()
        pc_cp.wait()
        pk_cp.wait()


def finish_body(x_v, ob_v, wo_v, cc_v, ckr_v, pc_v, pk_v, y_hbm, cco_hbm, ckro_hbm, y_v, sem):
    n = [0]

    def local(src, dst):
        cp = pltpu.make_async_copy(src, dst, sem.at[n[0]])
        n[0] += 1
        cp.start()
        return cp

    NB = 512
    outs = [
        local(cc_v.at[pl.ds(0, 4)], cco_hbm.at[pl.ds(0, 4)]),
        local(ckr_v.at[pl.ds(0, 4)], ckro_hbm.at[pl.ds(0, 4)]),
        local(pc_v, cco_hbm.at[4]),
        local(pk_v, ckro_hbm.at[4]),
    ]
    for j in range(DM // NB):
        cols = pl.ds(j * NB, NB)
        acc = jnp.dot(ob_v[...], wo_v[:, cols], preferred_element_type=F32)
        y_v[:, cols] = (x_v[:, cols].astype(F32) + acc).astype(BF)
        outs.append(local(y_v.at[:, cols], y_hbm.at[:, cols]))
    for cp in outs:
        cp.wait()


def finish(x, ob, wo, cc, ckr, pc, pk):
    any_spec = pl.BlockSpec(memory_space=pl.ANY)
    vm = pl.BlockSpec(memory_space=pltpu.VMEM)
    return pl.pallas_call(
        finish_body,
        name="mla_finish",
        out_shape=(
            jax.ShapeDtypeStruct((TOK, DM), BF),
            jax.ShapeDtypeStruct((5, TOK, LAT), BF),
            jax.ShapeDtypeStruct((5, TOK, RD), BF),
        ),
        in_specs=[vm] * 7,
        out_specs=(any_spec,) * 3,
        scratch_shapes=[
            pltpu.VMEM((TOK, DM), BF),
            pltpu.SemaphoreType.DMA((8,)),
        ],
        compiler_params=pltpu.CompilerParams(vmem_limit_bytes=16 * 1024 * 1024),
    )(x, ob, wo, cc, ckr, pc, pk)


def fused(x, tbl, wt, cc, ckr, wq, wdkv, g, wuk, wuv):
    any_spec = pl.BlockSpec(memory_space=pl.ANY)
    dma = pltpu.SemaphoreType.DMA
    return pl.pallas_call(
        body,
        name="mla_prefill",
        out_shape=(
            jax.ShapeDtypeStruct((TOK, DM), BF),
            jax.ShapeDtypeStruct((TOK, LAT), BF),
            jax.ShapeDtypeStruct((TOK, RD), BF),
        ),
        in_specs=[pl.BlockSpec(memory_space=pltpu.HBM)] * 10,
        out_specs=(any_spec,) * 3,
        scratch_shapes=[
            pltpu.VMEM((TOK, DM), BF),
            pltpu.VMEM((2, 256), jnp.int32),
            pltpu.SMEM((1, 2), jnp.int32),
            pltpu.VMEM((5, TOK, RD), BF),
            pltpu.VMEM((NGROUP, DM, GCOLS), BF),
            pltpu.VMEM((LAT + RD, DM), BF),
            pltpu.VMEM((LAT,), BF),
            pltpu.VMEM((LAT * NH, ND), BF),
            pltpu.VMEM((LAT * NH, ND), BF),
            pltpu.VMEM((8, 2, 2, TOK, LAT), BF),
            pltpu.VMEM((8, 2, TOK, 128), BF),
            pltpu.VMEM((8, 2, 32, LAT), BF),
            pltpu.VMEM((8, 48, 128), BF),
            pltpu.VMEM((NH, LAT, ND), BF),
            pltpu.VMEM((NH, LAT, ND), BF),
            pltpu.VMEM((ROWS, LAT), BF),
            pltpu.VMEM((NH, TOK, ND), BF),
            pltpu.VMEM((ROWS, 128), BF),
            pltpu.VMEM((2, BLK, 256), F32),
            pltpu.VMEM((ROWS, LAT), F32),
            pltpu.VMEM((ROWS, 128), F32),
            pltpu.VMEM((ROWS, 128), F32),
            pltpu.VMEM((8, 1, 256), F32),
            pltpu.VMEM((TOK, DM), BF),
            pltpu.VMEM((TOK, LAT), BF),
            pltpu.VMEM((TOK, RD), BF),
            dma((32,)),
            dma((NSEM,)),
            dma((NSEM,)),
        ],
        compiler_params=pltpu.CompilerParams(collective_id=0, has_side_effects=True, vmem_limit_bytes=40 * 1024 * 1024),
    )(*[pltpu.with_memory_space_constraint(a, pltpu.HBM) for a in (x, tbl, wt, cc, ckr, wq, wdkv, g, wuk, wuv)])


def solution(mesh):
    def device_step(hidden, pre_len, pre_table, wr_table, cache_c, cache_kr, w_q, w_dkv, g_kv, w_uk, w_uv, w_o):
        x = hidden.reshape(TOK, DM)
        ob, pc, pk = fused(
            x, pre_table.reshape(256, 2).T, wr_table.reshape(1, 2), cache_c[0], cache_kr[0],
            w_q, w_dkv.T, g_kv, w_uk.reshape(LAT * NH, ND), w_uv.reshape(LAT * NH, ND))
        y, c_out, kr_out = finish(x, ob, w_o, cache_c[0], cache_kr[0], pc, pk)
        return y[None], c_out[None], kr_out[None]

    row = P("pool")
    rep = P()
    return jax.shard_map(device_step, mesh=mesh, in_specs=(row,) * 6 + (rep,) * 6, out_specs=(row, row, row), check_vma=False)
```

```python
import contextlib
import math

import jax
import jax.numpy as jnp
import numpy as np
from jax import lax
from jax.experimental import pallas as pl
from jax.experimental.pallas import tpu as pltpu
from jax.sharding import PartitionSpec as P

BF = jnp.bfloat16
PROF = False
F32 = jnp.float32
MESH = pl.DeviceIdType.MESH

TOK = 64
DM = 2048
NH = 16
LAT = 512
RD = 64
ND = 128
HQ = ND + RD
ROWS = NH * TOK
EPS = 1e-6
GROUP = 4
GCOLS = GROUP * HQ
NB = 512
NGROUP = NH // GROUP
BLK = 256
SCALE2 = float((ND + RD) ** -0.5 * math.log2(math.e))
INV_FREQ = [float(np.float32(10000.0 ** (-k / 32.0))) for k in range(32)]

CHUNKS = (
    ((0, 0), (0, 1)),
    ((1, 0), (1, 1)),
    ((2, 0), (4, 1)),
    ((3, 0), (5, 1)),
    ((2, 1), (4, 0)),
    ((3, 1), (5, 0)),
    ((6, 0), (6, 1)),
    ((7, 0), (7, 1)),
)
HALF = 128 + 16
NEWR = TOK + 16

FLOWS = {
    "x0": (0, 0, 2, 0, "x"),
    "x1": (0, 1, 4, 0, "x"),
    "y1": (0, 1, 2, 1, "y"),
    "y0": (0, 0, 4, 1, "y"),
    "p0": (0, None, 1, None, "p"),
    "dy": (2, 0, 6, 0, "y"),
    "dx": (2, 1, 6, 1, "x"),
    "p2": (2, None, 3, None, "p"),
    "p4": (4, None, 5, None, "p"),
    "p6": (6, None, 7, None, "p"),
}
NEWS = {
    "nx": (0, 1, "x", 8),
    "ny": (0, 2, "y", 8),
    "nd": (0, 3, "d", 8),
    "np": (0, 4, "p", 9),
    "n1p": (1, 5, "p", 9),
    "n2p": (2, 6, "p", 9),
    "n3p": (3, 7, "p", 9),
}


def scope(name):
    return jax.named_scope(name) if PROF else contextlib.nullcontext()


def body(x_hbm, tbl_hbm, wt_hbm, cc_hbm, ckr_hbm, wq_hbm, wdkv_hbm, g_hbm, wuk_hbm, wuv_hbm, wo_hbm,
         y_v, pc_v, pk_v,
         x_v, tbl_v, wt_s, ckr_v, wq_v, wdkv_v, g_v, wuk_v, wuv_v, wo_v, ob_s,
         kc, nc, wukt, wuvt, q_s, qn_s, qr_s, s_s, p_s, a_s, o_s, m_s, l_s, bias_s,
         loc_sem, send_sem, recv_sem, diag_sem):
    me = lax.axis_index("pool")
    core = lax.rem(me, 2)
    cx = lax.rem(lax.div(me, 2), 2)
    cy = lax.div(me, 4)
    fp = 1 - 2 * core
    fx = 2 - 4 * cx
    fy = 4 - 8 * cy
    peer = {"p": me + fp, "x": me + fx, "y": me + fy, "d": me + fx + fy}

    barrier = pltpu.get_barrier_semaphore()
    for d in ("x", "y", "p"):
        pl.semaphore_signal(barrier, inc=1, device_id=(peer[d],), device_id_type=MESH)

    n_loc = [0]

    def local(src, dst):
        cp = pltpu.make_async_copy(src, dst, loc_sem.at[n_loc[0]])
        n_loc[0] += 1
        cp.start()
        return cp

    ld_kr = local(ckr_hbm.at[pl.ds(0, 4)], ckr_v)
    ld_c = [local(cc_hbm.at[pl.ds(128 * h, 128)], kc.at[0, h, pl.ds(0, 128)]) for h in range(2)]
    ld_tbl = local(tbl_hbm, tbl_v)
    ld_x = local(x_hbm, x_v)
    ld_dkv = local(wdkv_hbm, wdkv_v)
    ld_small = [local(wt_hbm, wt_s), local(g_hbm, g_v)]
    ld_uk = local(wuk_hbm, wuk_v)
    ld_q = [local(wq_hbm.at[:, pl.ds(g * GCOLS, GCOLS)], wq_v.at[g]) for g in range(NGROUP)]
    ld_uv = local(wuv_hbm, wuv_v)
    ld_o = local(wo_hbm, wo_v)

    lane = lax.broadcasted_iota(jnp.int32, (TOK, 128), 1)
    low = lane < RD

    ld_kr.wait()
    for h in range(2):
        kr = ckr_v[pl.ds(2 * h, 2)].reshape(128, RD)
        kc[0, h, pl.ds(128, 16), :] = jnp.concatenate([kr[16 * u:16 * u + 16] for u in range(8)], axis=-1)

    def half_of(c, h):
        return kc.at[c] if h is None else kc.at[c, h]

    def flow(name):
        if name in FLOWS:
            sc, sh, tc, th, d = FLOWS[name]
            src, dst, s_sem, r_sem = half_of(sc, sh), half_of(tc, th), send_sem.at[0], recv_sem.at[tc]
        else:
            ss, ts, d, r = NEWS[name]
            src, dst, s_sem, r_sem = nc.at[ss], nc.at[ts], send_sem.at[1], recv_sem.at[r]
        return pltpu.make_async_remote_copy(src_ref=src, dst_ref=dst, send_sem=s_sem, recv_sem=r_sem,
                                            device_id=(peer[d],), device_id_type=MESH)

    def sends(*names):
        for name in names:
            flow(name).start()

    def arrive(c):
        with scope(f"wait_c{c}"):
            pltpu.make_async_copy(kc.at[c], kc.at[c], recv_sem.at[c]).wait()

    def arrive_new(r):
        first, n = {8: (1, 3), 9: (4, 4)}[r]
        with scope(f"wait_n{r}"):
            pltpu.make_async_copy(nc.at[pl.ds(first, n)], nc.at[pl.ds(first, n)], recv_sem.at[r]).wait()

    with scope("tables"):
        ld_tbl.wait()
        k_lane = lax.rem(lane, 32)
        freq = jnp.zeros((TOK, 128), F32)
        for k, f in enumerate(INV_FREQ):
            freq = jnp.where(k_lane == k, f, freq)
        n_pages = jnp.sum(jnp.where(tbl_v[0:1] >= 0, 1.0, 0.0), axis=-1, keepdims=True)
        pos = lax.broadcasted_iota(jnp.int32, (TOK, 128), 0).astype(F32) + jnp.broadcast_to(n_pages * TOK, (TOK, 128))
        ang = pos * freq
        cos_t = jnp.cos(ang)
        sin_t = jnp.sin(ang)
        sin_t = jnp.where(lax.rem(lane, 64) < 32, -sin_t, sin_t)

    def rope2(v64):
        v = jnp.concatenate([v64, v64], axis=-1)
        return v * cos_t + pltpu.roll(v, 32, 1) * sin_t

    with scope("barrier"):
        pl.semaphore_wait(barrier, 3)
    pl.semaphore_signal(diag_sem, inc=1, device_id=(peer["x"],), device_id_type=MESH)
    with scope("send0"):
        for cp in ld_c:
            cp.wait()
        sends("x0", "y1", "p0", "x1", "y0")

    with scope("mult"):
        tbl = tbl_v[...]
        ids = (tbl[0:1] * 4 + tbl[1:2]).astype(F32)
        ids_col = jnp.transpose(jnp.broadcast_to(ids, (128, 256)))
        seg = lax.div(lax.broadcasted_iota(jnp.int32, (1, 256), 1), 64)
        flips = {0: 0, 1: fp, 2: fx, 4: fy, 3: fp + fx, 5: fp + fy, 6: fx + fy, 7: fp + fx + fy}
        for c, ((ra, ha), (rb, hb)) in enumerate(CHUNKS):
            pa = (me + flips[ra]) * 4 + 2 * ha
            pb = (me + flips[rb]) * 4 + 2 * hb
            want = jnp.where(seg == 0, pa, jnp.where(seg == 1, pa + 1, jnp.where(seg == 2, pb, pb + 1))).astype(F32)
            parts = []
            for t in range(2):
                hit = jnp.where(ids_col == want[:, t * 128:(t + 1) * 128], 1.0, 0.0)
                parts.append(jnp.sum(hit, axis=0, keepdims=True))
            cnt = jnp.concatenate(parts, axis=-1)
            bias_s[c] = jnp.where(cnt > 0.0, jnp.log2(jnp.maximum(cnt, 1.0)), -jnp.inf)

    with scope("newlat"):
        ld_x.wait()
        ld_dkv.wait()
        for cp in ld_small:
            cp.wait()
        kv = lax.dot_general(x_v[...], wdkv_v[...], (((1,), (1,)), ((), ())), preferred_element_type=F32)
        latp = kv[:, :LAT]
        inv_rms = lax.rsqrt(jnp.mean(latp * latp, axis=-1, keepdims=True) + EPS)
        nc[0, pl.ds(0, TOK), :] = (latp * inv_rms * g_v[...].astype(F32).reshape(1, LAT)).astype(BF)
        kr_dup = rope2(kv[:, LAT:])
        kr_low = jnp.where(low, kr_dup, 0.0).astype(BF)
        for u in range(2):
            pair = jnp.where(low[:16], kr_dup[32 * u:32 * u + 16], kr_dup[32 * u + 16:32 * u + 32])
            nc[0, pl.ds(TOK, 16), pl.ds(128 * u, 128)] = pair.astype(BF)
        nc[0, pl.ds(TOK, 16), pl.ds(256, 256)] = jnp.full((16, 256), wt_s[0, 0], jnp.int32).astype(F32).astype(BF)

    r_i = lax.broadcasted_iota(jnp.int32, (256, 256), 0)
    c_i = lax.broadcasted_iota(jnp.int32, (256, 256), 1)
    perm = (r_i == lax.rem(c_i, 16) * 16 + lax.div(c_i, 16)).astype(F32).astype(BF)

    def reorder(src, dst):
        for blk in range(0, 32, 2):
            rows = jnp.concatenate([src[pl.ds((blk + v) * 256, 256), :] for v in range(2)], axis=-1)
            t = jnp.dot(perm, rows, preferred_element_type=F32).astype(BF)
            for v in range(2):
                dst[:, pl.ds((blk + v) * 16, 16), :] = t[:, v * 128:(v + 1) * 128].reshape(NH, 16, 128)

    with scope("reorder_uk"):
        ld_uk.wait()
        reorder(wuk_v, wukt)

    def lift(g):
        for k in range(GROUP):
            h = g * GROUP + k
            q_s[pl.ds(h * TOK, TOK), :] = lax.dot_general(
                qn_s[h], wukt[h], (((1,), (1,)), ((), ())), preferred_element_type=F32).astype(BF)

    for g in range(NGROUP):
        with scope(f"waitq{g}"):
            ld_q[g].wait()
        with scope(f"query{g}"):
            qg = jnp.dot(x_v[...], wq_v[g], preferred_element_type=F32).astype(BF).astype(F32)
            if g:
                lift(g - 1)
            for k in range(GROUP):
                h = g * GROUP + k
                qn_s[h] = qg[:, k * HQ:k * HQ + ND].astype(BF)
                qr_s[pl.ds(h * TOK, TOK), :] = rope2(qg[:, k * HQ + ND:(k + 1) * HQ]).astype(BF)

    NT = (((1,), (1,)), ((), ()))
    row_tok = lax.rem(lax.broadcasted_iota(jnp.int32, (BLK, TOK), 0), TOK)
    causal = lax.broadcasted_iota(jnp.int32, (BLK, TOK), 1) <= row_tok
    lane16 = lax.broadcasted_iota(jnp.int32, (16, 128), 1) < RD

    def rope_keys(c):
        if c < 0:
            return kr_low
        out = []
        for h in range(2):
            for u in range(4):
                t = kc[c, h, pl.ds(128, 16), pl.ds(128 * u, 128)].astype(F32)
                out += [jnp.where(lane16, t, 0.0), jnp.where(lane16, 0.0, t)]
        return jnp.concatenate(out, axis=0).astype(BF)

    def keys_of(c):
        if c < 0:
            return nc[0, pl.ds(0, TOK), :]
        return jnp.concatenate([kc[c, h, pl.ds(0, 128), :] for h in range(2)], axis=0)

    def scores(c, b, slot, kbd):
        rows = pl.ds(b * BLK, BLK)
        s = lax.dot_general(q_s[rows, :], keys_of(c), NT, preferred_element_type=F32)
        s = s + lax.dot_general(qr_s[rows, :], kbd, NT, preferred_element_type=F32)
        if c < 0:
            s_s[slot, :, :TOK] = s
        else:
            s_s[slot] = s

    def weigh(c, b, slot):
        rows = pl.ds(b * BLK, BLK)
        if c < 0:
            t = jnp.where(causal, s_s[slot, :, :TOK] * SCALE2, -jnp.inf)
            mx = jnp.max(t, axis=-1, keepdims=True)
            p = jnp.exp2(t - mx)
            m_s[rows, :] = jnp.broadcast_to(mx, (BLK, 128))
            l_s[rows, :] = jnp.concatenate([p, jnp.zeros_like(p)], axis=-1)
            p_s[slot, :, :TOK] = p.astype(BF)
            return
        t = s_s[slot] * SCALE2 + bias_s[c]
        mx = jnp.max(jnp.maximum(t[:, :128], t[:, 128:]), axis=-1, keepdims=True)
        m_old = m_s[rows, :]
        m_new = jnp.maximum(m_old, jnp.broadcast_to(mx, (BLK, 128)))
        alpha = jnp.exp2(m_old - m_new)
        p = jnp.exp2(t - jnp.concatenate([m_new, m_new], axis=-1))
        m_s[rows, :] = m_new
        a_s[slot] = alpha
        l_s[rows, :] = l_s[rows, :] * alpha + (p[:, :128] + p[:, 128:])
        p_s[slot] = p.astype(BF)

    def combine(c, b, slot):
        rows = pl.ds(b * BLK, BLK)
        if c < 0:
            o_s[rows, :] = jnp.dot(p_s[slot, :, :TOK], keys_of(c), preferred_element_type=F32)
            return
        a4 = jnp.concatenate([a_s[slot]] * 4, axis=-1)
        o_s[rows, :] = o_s[rows, :] * a4 + jnp.dot(p_s[slot], keys_of(c), preferred_element_type=F32)

    def before(c):
        if c == -1:
            arrive(2)
            sends("dy", "dx", "p2", "nx", "ny", "np")
            pl.semaphore_wait(diag_sem, 1)
            sends("nd")
        elif c == 1:
            arrive(1)
        elif c == 3:
            arrive(3)
        elif c == 4:
            arrive(4)
            sends("p4")
        elif c == 5:
            arrive(5)
        elif c == 6:
            arrive(6)
            sends("p6")
        elif c == 7:
            with scope("reorder_uv"):
                ld_uv.wait()
                reorder(wuv_v, wuvt)
            arrive(7)

    seq = [(c, b) for c in (-1, 0, 1, 2, 4, 3, 5, 6, 7) for b in range(ROWS // BLK)]
    for n in range(len(seq) + 2):
        if n < len(seq) and seq[n][1] == 0:
            before(seq[n][0])
            kbd = rope_keys(seq[n][0])
        with scope(f"attend{seq[n][0] if n < len(seq) else 99}"):
            if n < len(seq):
                scores(*seq[n], n % 2, kbd)
            if n == 0:
                lift(NGROUP - 1)
            if n >= 2:
                combine(*seq[n - 2], n % 2)
            if 1 <= n <= len(seq):
                weigh(*seq[n - 1], (n - 1) % 2)

    with scope("values"):
        for h in range(NH):
            rows = pl.ds(h * TOK, TOK)
            denom = jnp.sum(l_s[rows, :], axis=-1, keepdims=True)
            ol = (o_s[rows, :] / denom).astype(BF)
            ob_s[:, pl.ds(h * ND, ND)] = jnp.dot(ol, wuvt[h], preferred_element_type=F32).astype(BF)

    arrive_new(8)
    sends("n1p", "n2p", "n3p")
    with scope("outproj"):
        ld_o.wait()
        for j in range(DM // NB):
            cols = pl.ds(j * NB, NB)
            acc = jnp.dot(ob_s[...], wo_v[:, cols], preferred_element_type=F32)
            y_v[:, cols] = (x_v[:, cols].astype(F32) + acc).astype(BF)

    arrive_new(9)
    with scope("page"):
        mine = me.astype(F32)
        page = jnp.zeros((TOK, LAT), F32)
        packed = jnp.zeros((16, 256), F32)
        for r in range(8):
            hit = nc[r, pl.ds(TOK, 16), pl.ds(256, 256)].astype(F32) == mine
            packed = jnp.where(hit, nc[r, pl.ds(TOK, 16), pl.ds(0, 256)].astype(F32), packed)
            hit = jnp.concatenate([jnp.concatenate([hit] * 2, axis=-1)] * 4, axis=0)
            page = jnp.where(hit, nc[r, pl.ds(0, TOK), :].astype(F32), page)
        pc_v[...] = page.astype(BF)
        packed = packed.astype(BF)
        for u in range(4):
            pk_v[pl.ds(16 * u, 16), :] = packed[:, RD * u:RD * (u + 1)]
    with scope("final_wait"):
        pltpu.make_async_copy(kc.at[pl.ds(0, 7)], kc.at[pl.ds(0, 7)], send_sem.at[0]).wait()
        pltpu.make_async_copy(nc.at[pl.ds(0, 7)], nc.at[pl.ds(0, 7)], send_sem.at[1]).wait()


def finish_body(y_v, cc_v, ckr_v, pc_v, pk_v, y_hbm, cco_hbm, ckro_hbm, sem):
    copies = [
        pltpu.make_async_copy(src, dst, sem.at[n]) for n, (src, dst) in enumerate([
            (y_v, y_hbm),
            (cc_v.at[pl.ds(0, 4)], cco_hbm.at[pl.ds(0, 4)]),
            (pc_v, cco_hbm.at[4]),
            (ckr_v.at[pl.ds(0, 4)], ckro_hbm.at[pl.ds(0, 4)]),
            (pk_v, ckro_hbm.at[4]),
        ])
    ]
    for cp in copies:
        cp.start()
    for cp in copies:
        cp.wait()


def finish(y, cc, ckr, pc, pk):
    return pl.pallas_call(
        finish_body,
        name="mla_finish",
        out_shape=(
            jax.ShapeDtypeStruct((TOK, DM), BF),
            jax.ShapeDtypeStruct((5, TOK, LAT), BF),
            jax.ShapeDtypeStruct((5, TOK, RD), BF),
        ),
        in_specs=[pl.BlockSpec(memory_space=pltpu.VMEM)] * 5,
        out_specs=(pl.BlockSpec(memory_space=pl.ANY),) * 3,
        scratch_shapes=[pltpu.SemaphoreType.DMA((5,))],
        compiler_params=pltpu.CompilerParams(vmem_limit_bytes=4 * 1024 * 1024),
    )(y, cc, ckr, pc, pk)


def fused(*args):
    dma = pltpu.SemaphoreType.DMA
    args = [pltpu.with_memory_space_constraint(a, pltpu.HBM) for a in args]
    return pl.pallas_call(
        body,
        name="mla_prefill",
        out_shape=(
            jax.ShapeDtypeStruct((TOK, DM), BF),
            jax.ShapeDtypeStruct((TOK, LAT), BF),
            jax.ShapeDtypeStruct((TOK, RD), BF),
        ),
        in_specs=[pl.BlockSpec(memory_space=pltpu.HBM)] * len(args),
        out_specs=(pl.BlockSpec(memory_space=pltpu.VMEM),) * 3,
        scratch_shapes=[
            pltpu.VMEM((TOK, DM), BF),
            pltpu.VMEM((2, 256), jnp.int32),
            pltpu.SMEM((1, 2), jnp.int32),
            pltpu.VMEM((4, TOK, RD), BF),
            pltpu.VMEM((NGROUP, DM, GCOLS), BF),
            pltpu.VMEM((LAT + RD, DM), BF),
            pltpu.VMEM((LAT,), BF),
            pltpu.VMEM((LAT * NH, ND), BF),
            pltpu.VMEM((LAT * NH, ND), BF),
            pltpu.VMEM((DM, DM), BF),
            pltpu.VMEM((TOK, DM), BF),
            pltpu.VMEM((8, 2, HALF, LAT), BF),
            pltpu.VMEM((8, NEWR, LAT), BF),
            pltpu.VMEM((NH, LAT, ND), BF),
            pltpu.VMEM((NH, LAT, ND), BF),
            pltpu.VMEM((ROWS, LAT), BF),
            pltpu.VMEM((NH, TOK, ND), BF),
            pltpu.VMEM((ROWS, 128), BF),
            pltpu.VMEM((2, BLK, 256), F32),
            pltpu.VMEM((2, BLK, 256), BF),
            pltpu.VMEM((2, BLK, 128), F32),
            pltpu.VMEM((ROWS, LAT), F32),
            pltpu.VMEM((ROWS, 128), F32),
            pltpu.VMEM((ROWS, 128), F32),
            pltpu.VMEM((8, 1, 256), F32),
            dma((15,)),
            dma((2,)),
            dma((10,)),
            pltpu.SemaphoreType.REGULAR,
        ],
        compiler_params=pltpu.CompilerParams(collective_id=0, has_side_effects=True, vmem_limit_bytes=50 * 1024 * 1024),
    )(*args)


def solution(mesh):
    def device_step(hidden, pre_len, pre_table, wr_table, cache_c, cache_kr, w_q, w_dkv, g_kv, w_uk, w_uv, w_o):
        y, pc, pk = fused(
            hidden.reshape(TOK, DM), pre_table.reshape(256, 2).T, wr_table.reshape(1, 2), cache_c.reshape(5 * TOK, LAT), cache_kr[0],
            w_q, w_dkv.T, g_kv, w_uk.reshape(LAT * NH, ND), w_uv.reshape(LAT * NH, ND), w_o)
        y, c_out, kr_out = finish(y, cache_c[0], cache_kr[0], pc, pk)
        return y[None], c_out[None], kr_out[None]

    row = P("pool")
    rep = P()
    return jax.shard_map(device_step, mesh=mesh, in_specs=(row,) * 6 + (rep,) * 6, out_specs=(row, row, row), check_vma=False)
```

```python
import contextlib
import math

import jax
import jax.numpy as jnp
import numpy as np
from jax import lax
from jax.experimental import pallas as pl
from jax.experimental.pallas import tpu as pltpu
from jax.sharding import PartitionSpec as P

BF = jnp.bfloat16
PROF = False
F32 = jnp.float32
MESH = pl.DeviceIdType.MESH

TOK = 64
DM = 2048
NH = 16
LAT = 512
RD = 64
ND = 128
HQ = ND + RD
ROWS = NH * TOK
EPS = 1e-6
GROUP = 4
GCOLS = GROUP * HQ
NB = 512
NGROUP = NH // GROUP
BLK = 256
NBLK = ROWS // BLK
SCALE2 = float((ND + RD) ** -0.5 * math.log2(math.e))
INV_FREQ = [float(np.float32(10000.0 ** (-k / 32.0))) for k in range(32)]

CHUNKS = (
    ((0, 0), (0, 1)),
    ((1, 0), (1, 1)),
    ((2, 0), (4, 1)),
    ((3, 0), (5, 1)),
    ((2, 1), (4, 0)),
    ((3, 1), (5, 0)),
    ((6, 0), (6, 1)),
    ((7, 0), (7, 1)),
)
HALF = 128 + 16
NEWR = TOK + 16

FLOWS = {
    "x0": (0, 0, 2, 0, "x"),
    "x1": (0, 1, 4, 0, "x"),
    "y1": (0, 1, 2, 1, "y"),
    "y0": (0, 0, 4, 1, "y"),
    "p0": (0, None, 1, None, "p"),
    "dy": (2, 0, 6, 0, "y"),
    "dx": (2, 1, 6, 1, "x"),
    "p2": (2, None, 3, None, "p"),
    "p4": (4, None, 5, None, "p"),
    "p6": (6, None, 7, None, "p"),
}
NEWS = {
    "nx": (0, 1, "x", 8),
    "ny": (0, 2, "y", 8),
    "nd": (0, 3, "d", 10),
    "np": (0, 4, "p", 9),
    "n1p": (1, 5, "p", 9),
    "n2p": (2, 6, "p", 9),
    "n3p": (3, 7, "p", 9),
}


def scope(name):
    return jax.named_scope(name) if PROF else contextlib.nullcontext()


def body(x_hbm, tbl_hbm, wt_hbm, cc_hbm, ckr_hbm, wq_hbm, wdkv_hbm, g_hbm, wuk_hbm, wuv_hbm, wo_hbm,
         y_v, pc_v, pk_v,
         x_v, tbl_v, wt_s, ckr_v, wq_v, wdkv_v, g_v, wuk_v, wuv_v, wo_v, ob_s, y_acc,
         kc, nc, wukt, wuvt, q_s, qraw_s, qn_s, qr_s, s_s, p_s, a_s, o_s, m_s, l_s, bias_s,
         loc_sem, send_sem, recv_sem, diag_sem):
    me = lax.axis_index("pool")
    core = lax.rem(me, 2)
    cx = lax.rem(lax.div(me, 2), 2)
    cy = lax.div(me, 4)
    fp = 1 - 2 * core
    fx = 2 - 4 * cx
    fy = 4 - 8 * cy
    peer = {"p": me + fp, "x": me + fx, "y": me + fy, "d": me + fx + fy}

    barrier = pltpu.get_barrier_semaphore()
    for d in ("x", "y", "p"):
        pl.semaphore_signal(barrier, inc=1, device_id=(peer[d],), device_id_type=MESH)

    n_loc = [0]

    def local(src, dst):
        cp = pltpu.make_async_copy(src, dst, loc_sem.at[n_loc[0]])
        n_loc[0] += 1
        cp.start()
        return cp

    ld_kr = local(ckr_hbm.at[pl.ds(0, 4)], ckr_v)
    ld_c = [local(cc_hbm.at[pl.ds(128 * h, 128)], kc.at[0, h, pl.ds(0, 128)]) for h in range(2)]
    ld_tbl = local(tbl_hbm, tbl_v)
    ld_x = local(x_hbm, x_v.at[pl.ds(0, TOK)])
    ld_dkv = local(wdkv_hbm, wdkv_v)
    ld_small = [local(wt_hbm, wt_s), local(g_hbm, g_v)]
    ld_uk = local(wuk_hbm, wuk_v)
    ld_q = [local(wq_hbm.at[:, pl.ds(g * GCOLS, GCOLS)], wq_v.at[g]) for g in range(NGROUP)]
    ld_uv = local(wuv_hbm, wuv_v)
    ld_o = local(wo_hbm, wo_v)

    x_v[pl.ds(TOK, TOK), :] = jnp.zeros((TOK, DM), BF)
    for b in range(NBLK):
        ob_s[b, pl.ds(TOK, TOK), :] = jnp.zeros((TOK, GROUP * ND), BF)
    for pr in range(NH // 2):
        qn_s[pr, pl.ds(0, TOK), pl.ds(ND, ND)] = jnp.zeros((TOK, ND), BF)
        qn_s[pr, pl.ds(TOK, TOK), pl.ds(0, ND)] = jnp.zeros((TOK, ND), BF)
    lane = lax.broadcasted_iota(jnp.int32, (TOK, 128), 1)
    low = lane < RD

    ld_kr.wait()
    for h in range(2):
        kr = ckr_v[pl.ds(2 * h, 2)].reshape(128, RD)
        kc[0, h, pl.ds(128, 16), :] = jnp.concatenate([kr[16 * u:16 * u + 16] for u in range(8)], axis=-1)

    def half_of(c, h):
        return kc.at[c] if h is None else kc.at[c, h]

    def flow(name):
        if name in FLOWS:
            sc, sh, tc, th, d = FLOWS[name]
            src, dst, s_sem, r_sem = half_of(sc, sh), half_of(tc, th), send_sem.at[0], recv_sem.at[tc]
        else:
            ss, ts, d, r = NEWS[name]
            src, dst, s_sem, r_sem = nc.at[ss], nc.at[ts], send_sem.at[1], recv_sem.at[r]
        return pltpu.make_async_remote_copy(src_ref=src, dst_ref=dst, send_sem=s_sem, recv_sem=r_sem,
                                            device_id=(peer[d],), device_id_type=MESH)

    def sends(*names):
        for name in names:
            flow(name).start()

    def arrive(c):
        with scope(f"wait_c{c}"):
            pltpu.make_async_copy(kc.at[c], kc.at[c], recv_sem.at[c]).wait()

    def arrive_new(r):
        first, n = {8: (1, 2), 10: (3, 1), 9: (4, 4)}[r]
        with scope(f"wait_n{r}"):
            pltpu.make_async_copy(nc.at[pl.ds(first, n)], nc.at[pl.ds(first, n)], recv_sem.at[r]).wait()

    with scope("tables"):
        ld_tbl.wait()
        k_lane = lax.rem(lane, 32)
        freq = jnp.zeros((TOK, 128), F32)
        for k, f in enumerate(INV_FREQ):
            freq = jnp.where(k_lane == k, f, freq)
        n_pages = jnp.sum(jnp.where(tbl_v[0:1] >= 0, 1.0, 0.0), axis=-1, keepdims=True)
        pos = lax.broadcasted_iota(jnp.int32, (TOK, 128), 0).astype(F32) + jnp.broadcast_to(n_pages * TOK, (TOK, 128))
        ang = pos * freq
        cos_t = jnp.cos(ang)
        sin_t = jnp.sin(ang)
        sin_t = jnp.where(lax.rem(lane, 64) < 32, -sin_t, sin_t)

    def rope2(v64):
        v = jnp.concatenate([v64, v64], axis=-1)
        return v * cos_t + pltpu.roll(v, 32, 1) * sin_t

    with scope("barrier"):
        pl.semaphore_wait(barrier, 3)
    pl.semaphore_signal(diag_sem, inc=1, device_id=(peer["x"],), device_id_type=MESH)
    with scope("send0"):
        for cp in ld_c:
            cp.wait()
        sends("x0", "y1", "p0", "x1", "y0")

    with scope("mult"):
        tbl = tbl_v[...]
        ids = (tbl[0:1] * 4 + tbl[1:2]).astype(F32)
        ids_col = jnp.transpose(jnp.broadcast_to(ids, (128, 256)))
        seg = lax.div(lax.broadcasted_iota(jnp.int32, (1, 256), 1), 64)
        flips = {0: 0, 1: fp, 2: fx, 4: fy, 3: fp + fx, 5: fp + fy, 6: fx + fy, 7: fp + fx + fy}
        for c, ((ra, ha), (rb, hb)) in enumerate(CHUNKS):
            pa = (me + flips[ra]) * 4 + 2 * ha
            pb = (me + flips[rb]) * 4 + 2 * hb
            want = jnp.where(seg == 0, pa, jnp.where(seg == 1, pa + 1, jnp.where(seg == 2, pb, pb + 1))).astype(F32)
            parts = []
            for t in range(2):
                hit = jnp.where(ids_col == want[:, t * 128:(t + 1) * 128], 1.0, 0.0)
                parts.append(jnp.sum(hit, axis=0, keepdims=True))
            cnt = jnp.concatenate(parts, axis=-1)
            bias_s[c] = jnp.where(cnt > 0.0, jnp.log2(jnp.maximum(cnt, 1.0)), -jnp.inf)

    with scope("newlat"):
        ld_x.wait()
        ld_dkv.wait()
        for cp in ld_small:
            cp.wait()
        kv = lax.dot_general(x_v[pl.ds(0, TOK), :], wdkv_v[...], (((1,), (1,)), ((), ())), preferred_element_type=F32)
        latp = kv[:, :LAT]
        inv_rms = lax.rsqrt(jnp.mean(latp * latp, axis=-1, keepdims=True) + EPS)
        nc[0, pl.ds(0, TOK), :] = (latp * inv_rms * g_v[...].astype(F32).reshape(1, LAT)).astype(BF)
        kr_dup = rope2(kv[:, LAT:])
        kr_low = jnp.where(low, kr_dup, 0.0).astype(BF)
        for u in range(2):
            pair = jnp.where(low[:16], kr_dup[32 * u:32 * u + 16], kr_dup[32 * u + 16:32 * u + 32])
            nc[0, pl.ds(TOK, 16), pl.ds(128 * u, 128)] = pair.astype(BF)
        nc[0, pl.ds(TOK, 16), pl.ds(256, 256)] = jnp.full((16, 256), wt_s[0, 0], jnp.int32).astype(F32).astype(BF)

    r_i = lax.broadcasted_iota(jnp.int32, (256, 256), 0)
    c_i = lax.broadcasted_iota(jnp.int32, (256, 256), 1)
    perm = (r_i == lax.rem(c_i, 16) * 16 + lax.div(c_i, 16)).astype(F32).astype(BF)

    def reorder(src, dst):
        for blk in range(0, 32, 2):
            rows = jnp.concatenate([src[pl.ds((blk + v) * 256, 256), :] for v in range(2)], axis=-1)
            t = jnp.dot(perm, rows, preferred_element_type=F32).astype(BF)
            for v in range(2):
                for h in range(NH):
                    dst[h // 2, pl.ds((blk + v) * 16, 16), pl.ds((h % 2) * ND, ND)] = t[16 * h:16 * h + 16, v * 128:(v + 1) * 128]

    with scope("reorder_uk"):
        ld_uk.wait()
        reorder(wuk_v, wukt)

    def lift(g):
        for pr in range(g * GROUP // 2, (g + 1) * GROUP // 2):
            q_s[pl.ds(pr * 2 * TOK, 2 * TOK), :] = lax.dot_general(
                qn_s[pr], wukt[pr], (((1,), (1,)), ((), ())), preferred_element_type=F32).astype(BF)

    def post(g):
        qg = qraw_s[g % 2].astype(BF).astype(F32)
        for k in range(GROUP):
            h = g * GROUP + k
            qn_s[h // 2, pl.ds((h % 2) * TOK, TOK), pl.ds((h % 2) * ND, ND)] = qg[:, k * HQ:k * HQ + ND].astype(BF)
            qr_s[pl.ds(h * TOK, TOK), :] = rope2(qg[:, k * HQ + ND:(k + 1) * HQ]).astype(BF)

    for g in range(NGROUP):
        with scope(f"waitq{g}"):
            ld_q[g].wait()
        with scope(f"query{g}"):
            qraw_s[g % 2] = jnp.dot(x_v[...], wq_v[g], preferred_element_type=F32)[:TOK]
            if g:
                post(g - 1)
                lift(g - 1)
    with scope("reorder_uv"):
        ld_uv.wait()
        reorder(wuv_v, wuvt)

    NT = (((1,), (1,)), ((), ()))
    row_tok = lax.rem(lax.broadcasted_iota(jnp.int32, (BLK, TOK), 0), TOK)
    causal = lax.broadcasted_iota(jnp.int32, (BLK, TOK), 1) <= row_tok
    lane16 = lax.broadcasted_iota(jnp.int32, (16, 128), 1) < RD

    def rope_keys(c):
        if c < 0:
            return kr_low
        out = []
        for h in range(2):
            for u in range(4):
                t = kc[c, h, pl.ds(128, 16), pl.ds(128 * u, 128)].astype(F32)
                out += [jnp.where(lane16, t, 0.0), jnp.where(lane16, 0.0, t)]
        return jnp.concatenate(out, axis=0).astype(BF)

    def keys_of(c):
        if c < 0:
            return nc[0, pl.ds(0, TOK), :]
        return jnp.concatenate([kc[c, h, pl.ds(0, 128), :] for h in range(2)], axis=0)

    def scores(c, b, slot, kbd):
        rows = pl.ds(b * BLK, BLK)
        s = lax.dot_general(q_s[rows, :], keys_of(c), NT, preferred_element_type=F32)
        s = s + lax.dot_general(qr_s[rows, :], kbd, NT, preferred_element_type=F32)
        if c < 0:
            s_s[slot, :, :TOK] = s
        else:
            s_s[slot] = s

    def weigh(c, b, slot):
        rows = pl.ds(b * BLK, BLK)
        if c < 0:
            t = jnp.where(causal, s_s[slot, :, :TOK] * SCALE2, -jnp.inf)
            mx = jnp.max(t, axis=-1, keepdims=True)
            p = jnp.exp2(t - mx)
            m_s[rows, :] = jnp.broadcast_to(mx, (BLK, 128))
            l_s[rows, :] = jnp.concatenate([p, jnp.zeros_like(p)], axis=-1)
            p_s[slot, :, :TOK] = p.astype(BF)
            return
        t = s_s[slot] * SCALE2 + bias_s[c]
        mx = jnp.max(jnp.maximum(t[:, :128], t[:, 128:]), axis=-1, keepdims=True)
        m_old = m_s[rows, :]
        m_new = jnp.maximum(m_old, jnp.broadcast_to(mx, (BLK, 128)))
        alpha = jnp.exp2(m_old - m_new)
        p = jnp.exp2(t - jnp.concatenate([m_new, m_new], axis=-1))
        m_s[rows, :] = m_new
        a_s[slot] = alpha
        l_s[rows, :] = l_s[rows, :] * alpha + (p[:, :128] + p[:, 128:])
        p_s[slot] = p.astype(BF)

    def combine(c, b, slot):
        rows = pl.ds(b * BLK, BLK)
        if c < 0:
            o_s[rows, :] = jnp.dot(p_s[slot, :, :TOK], keys_of(c), preferred_element_type=F32)
            return
        a4 = jnp.concatenate([a_s[slot]] * 4, axis=-1)
        o_s[rows, :] = o_s[rows, :] * a4 + jnp.dot(p_s[slot], keys_of(c), preferred_element_type=F32)

    def values(b):
        for pr in range(b * GROUP // 2, (b + 1) * GROUP // 2):
            rows = pl.ds(pr * 2 * TOK, 2 * TOK)
            denom = jnp.sum(l_s[rows, :], axis=-1, keepdims=True)
            ol = (o_s[rows, :] / denom).astype(BF)
            val = jnp.dot(ol, wuvt[pr], preferred_element_type=F32).astype(BF)
            ob_s[b, pl.ds(0, TOK), pl.ds((pr * 2 - b * GROUP) * ND, ND)] = val[:TOK, :ND]
            ob_s[b, pl.ds(0, TOK), pl.ds((pr * 2 - b * GROUP) * ND + ND, ND)] = val[TOK:, ND:]

    def project(b):
        deep = pl.ds(b * GROUP * ND, GROUP * ND)
        for j in range(DM // NB):
            cols = pl.ds(j * NB, NB)
            part = jnp.dot(ob_s[b], wo_v[deep, cols], preferred_element_type=F32)[:TOK]
            if b == 0:
                y_acc[:, cols] = x_v[pl.ds(0, TOK), cols].astype(F32) + part
            elif b < NBLK - 1:
                y_acc[:, cols] = y_acc[:, cols] + part
            else:
                y_v[:, cols] = (y_acc[:, cols] + part).astype(BF)

    def pass_on(which, r, *names):
        @pl.when(core == which)
        def _():
            arrive_new(r)
            sends(*names)

    def before(c):
        if c == -1:
            arrive(2)
            sends("dy", "dx", "p2", "nx", "ny", "np")
            pl.semaphore_wait(diag_sem, 1)
            sends("nd")
        elif c == 1:
            arrive(1)
        elif c == 3:
            arrive(3)
        elif c == 4:
            arrive(4)
            sends("p4")
        elif c == 5:
            arrive(5)
        elif c == 6:
            arrive(6)
            sends("p6")
        elif c == 7:
            arrive(7)
            pass_on(1, 8, "n1p", "n2p")

    seq = [(c, b) for c in (-1, 0, 1, 2, 4, 3, 5, 6, 7) for b in range(NBLK)]
    end = len(seq)
    for n in range(end + 4):
        if n < end and seq[n][1] == 0:
            before(seq[n][0])
            kbd = rope_keys(seq[n][0])
        if n == end:
            ld_o.wait()
            pass_on(1, 10, "n3p")
            pass_on(0, 8, "n1p", "n2p")
        with scope(f"attend{seq[n][0] if n < end else 99}") if n < end else contextlib.nullcontext():
            if n < end:
                scores(*seq[n], n % 2, kbd)
            if n == 0:
                post(NGROUP - 1)
                lift(NGROUP - 1)
            if 2 <= n < end + 2:
                combine(*seq[n - 2], n % 2)
            if 1 <= n <= end:
                weigh(*seq[n - 1], (n - 1) % 2)
            if end - NBLK <= n - 3 < end:
                values(seq[n - 3][1])
            if end - NBLK <= n - 4 < end:
                project(seq[n - 4][1])
    pass_on(0, 10, "n3p")
    with scope("tail"):
        project(NBLK - 1)

    arrive_new(9)
    with scope("page"):
        mine = me.astype(F32)
        page = jnp.zeros((TOK, LAT), F32)
        packed = jnp.zeros((16, 256), F32)
        for r in range(8):
            hit = nc[r, pl.ds(TOK, 16), pl.ds(256, 256)].astype(F32) == mine
            packed = jnp.where(hit, nc[r, pl.ds(TOK, 16), pl.ds(0, 256)].astype(F32), packed)
            hit = jnp.concatenate([jnp.concatenate([hit] * 2, axis=-1)] * 4, axis=0)
            page = jnp.where(hit, nc[r, pl.ds(0, TOK), :].astype(F32), page)
        pc_v[...] = page.astype(BF)
        packed = packed.astype(BF)
        for u in range(4):
            pk_v[pl.ds(16 * u, 16), :] = packed[:, RD * u:RD * (u + 1)]
    with scope("final_wait"):
        pltpu.make_async_copy(kc.at[pl.ds(0, 7)], kc.at[pl.ds(0, 7)], send_sem.at[0]).wait()
        pltpu.make_async_copy(nc.at[pl.ds(0, 7)], nc.at[pl.ds(0, 7)], send_sem.at[1]).wait()


def finish_body(y_v, cc_v, ckr_v, pc_v, pk_v, y_hbm, cco_hbm, ckro_hbm, sem):
    copies = [
        pltpu.make_async_copy(src, dst, sem.at[n]) for n, (src, dst) in enumerate([
            (y_v, y_hbm),
            (cc_v.at[pl.ds(0, 4)], cco_hbm.at[pl.ds(0, 4)]),
            (pc_v, cco_hbm.at[4]),
            (ckr_v.at[pl.ds(0, 4)], ckro_hbm.at[pl.ds(0, 4)]),
            (pk_v, ckro_hbm.at[4]),
        ])
    ]
    for cp in copies:
        cp.start()
    for cp in copies:
        cp.wait()


def finish(y, cc, ckr, pc, pk):
    return pl.pallas_call(
        finish_body,
        name="mla_finish",
        out_shape=(
            jax.ShapeDtypeStruct((TOK, DM), BF),
            jax.ShapeDtypeStruct((5, TOK, LAT), BF),
            jax.ShapeDtypeStruct((5, TOK, RD), BF),
        ),
        in_specs=[pl.BlockSpec(memory_space=pltpu.VMEM)] * 5,
        out_specs=(pl.BlockSpec(memory_space=pl.ANY),) * 3,
        scratch_shapes=[pltpu.SemaphoreType.DMA((5,))],
        compiler_params=pltpu.CompilerParams(vmem_limit_bytes=4 * 1024 * 1024),
    )(y, cc, ckr, pc, pk)


def fused(*args):
    dma = pltpu.SemaphoreType.DMA
    args = [pltpu.with_memory_space_constraint(a, pltpu.HBM) for a in args]
    return pl.pallas_call(
        body,
        name="mla_prefill",
        out_shape=(
            jax.ShapeDtypeStruct((TOK, DM), BF),
            jax.ShapeDtypeStruct((TOK, LAT), BF),
            jax.ShapeDtypeStruct((TOK, RD), BF),
        ),
        in_specs=[pl.BlockSpec(memory_space=pltpu.HBM)] * len(args),
        out_specs=(pl.BlockSpec(memory_space=pltpu.VMEM),) * 3,
        scratch_shapes=[
            pltpu.VMEM((2 * TOK, DM), BF),
            pltpu.VMEM((2, 256), jnp.int32),
            pltpu.SMEM((1, 2), jnp.int32),
            pltpu.VMEM((4, TOK, RD), BF),
            pltpu.VMEM((NGROUP, DM, GCOLS), BF),
            pltpu.VMEM((LAT + RD, DM), BF),
            pltpu.VMEM((LAT,), BF),
            pltpu.VMEM((LAT * NH, ND), BF),
            pltpu.VMEM((LAT * NH, ND), BF),
            pltpu.VMEM((DM, DM), BF),
            pltpu.VMEM((NBLK, 2 * TOK, GROUP * ND), BF),
            pltpu.VMEM((TOK, DM), F32),
            pltpu.VMEM((8, 2, HALF, LAT), BF),
            pltpu.VMEM((8, NEWR, LAT), BF),
            pltpu.VMEM((NH // 2, LAT, 2 * ND), BF),
            pltpu.VMEM((NH // 2, LAT, 2 * ND), BF),
            pltpu.VMEM((ROWS, LAT), BF),
            pltpu.VMEM((2, TOK, GCOLS), F32),
            pltpu.VMEM((NH // 2, 2 * TOK, 2 * ND), BF),
            pltpu.VMEM((ROWS, 128), BF),
            pltpu.VMEM((2, BLK, 256), F32),
            pltpu.VMEM((2, BLK, 256), BF),
            pltpu.VMEM((2, BLK, 128), F32),
            pltpu.VMEM((ROWS, LAT), F32),
            pltpu.VMEM((ROWS, 128), F32),
            pltpu.VMEM((ROWS, 128), F32),
            pltpu.VMEM((8, 1, 256), F32),
            dma((15,)),
            dma((2,)),
            dma((11,)),
            pltpu.SemaphoreType.REGULAR,
        ],
        compiler_params=pltpu.CompilerParams(collective_id=0, has_side_effects=True, vmem_limit_bytes=50 * 1024 * 1024),
    )(*args)


def solution(mesh):
    def device_step(hidden, pre_len, pre_table, wr_table, cache_c, cache_kr, w_q, w_dkv, g_kv, w_uk, w_uv, w_o):
        y, pc, pk = fused(
            hidden.reshape(TOK, DM), pre_table.reshape(256, 2).T, wr_table.reshape(1, 2), cache_c.reshape(5 * TOK, LAT), cache_kr[0],
            w_q, w_dkv.T, g_kv, w_uk.reshape(LAT * NH, ND), w_uv.reshape(LAT * NH, ND), w_o)
        y, c_out, kr_out = finish(y, cache_c[0], cache_kr[0], pc, pk)
        return y[None], c_out[None], kr_out[None]

    row = P("pool")
    rep = P()
    return jax.shard_map(device_step, mesh=mesh, in_specs=(row,) * 6 + (rep,) * 6, out_specs=(row, row, row), check_vma=False)
```

```python
import contextlib
import math

import jax
import jax.numpy as jnp
import numpy as np
from jax import lax
from jax.experimental import pallas as pl
from jax.experimental.pallas import tpu as pltpu
from jax.sharding import PartitionSpec as P

BF = jnp.bfloat16
PROF = False
F32 = jnp.float32
MESH = pl.DeviceIdType.MESH

TOK = 64
DM = 2048
NH = 16
LAT = 512
RD = 64
ND = 128
HQ = ND + RD
ROWS = NH * TOK
EPS = 1e-6
GROUP = 4
GCOLS = GROUP * HQ
NB = 512
NGROUP = NH // GROUP
BLK = 256
NBLK = ROWS // BLK
SCALE2 = float((ND + RD) ** -0.5 * math.log2(math.e))
INV_FREQ = [float(np.float32(10000.0 ** (-k / 32.0))) for k in range(32)]

CHUNKS = (
    ((0, 0), (0, 1)),
    ((1, 0), (1, 1)),
    ((2, 0), (4, 1)),
    ((3, 0), (5, 1)),
    ((2, 1), (4, 0)),
    ((3, 1), (5, 0)),
    ((6, 0), (6, 1)),
    ((7, 0), (7, 1)),
)
HALF = 128 + 16
NEWR = TOK + 16

FLOWS = {
    "x0": (0, 0, 2, 0, "x"),
    "x1": (0, 1, 4, 0, "x"),
    "y1": (0, 1, 2, 1, "y"),
    "y0": (0, 0, 4, 1, "y"),
    "p0": (0, None, 1, None, "p"),
    "dy": (2, 0, 6, 0, "y"),
    "dx": (2, 1, 6, 1, "x"),
    "p2": (2, None, 3, None, "p"),
    "p4": (4, None, 5, None, "p"),
    "p6": (6, None, 7, None, "p"),
}
NEWS = {
    "nx": (0, 1, "x", 8),
    "ny": (0, 2, "y", 8),
    "nd": (0, 3, "d", 10),
    "np": (0, 4, "p", 9),
    "n1p": (1, 5, "p", 9),
    "n2p": (2, 6, "p", 9),
    "n3p": (3, 7, "p", 9),
}


def scope(name):
    return jax.named_scope(name) if PROF else contextlib.nullcontext()


def body(x_hbm, tbl_hbm, wt_hbm, cc_hbm, ckr_hbm, wq_hbm, wdkv_hbm, g_hbm, wuk_hbm, wuv_hbm, wo_hbm,
         y_v, pc_v, pk_v,
         x_v, tbl_v, wt_s, ckr_v, wq_v, wdkv_v, g_v, wuk_v, wuv_v, wo_v, ob_s, y_acc,
         kc, nc, wukt, wuvt, q_s, qraw_s, qn_s, qr_s, s_s, p_s, a_s, o_s, m_s, l_s, bias_s,
         loc_sem, send_sem, recv_sem, diag_sem):
    me = lax.axis_index("pool")
    core = lax.rem(me, 2)
    cx = lax.rem(lax.div(me, 2), 2)
    cy = lax.div(me, 4)
    fp = 1 - 2 * core
    fx = 2 - 4 * cx
    fy = 4 - 8 * cy
    peer = {"p": me + fp, "x": me + fx, "y": me + fy, "d": me + fx + fy}

    barrier = pltpu.get_barrier_semaphore()
    for d in ("x", "y", "p"):
        pl.semaphore_signal(barrier, inc=1, device_id=(peer[d],), device_id_type=MESH)

    n_loc = [0]

    def local(src, dst):
        cp = pltpu.make_async_copy(src, dst, loc_sem.at[n_loc[0]])
        n_loc[0] += 1
        cp.start()
        return cp

    ld_kr = local(ckr_hbm.at[pl.ds(0, 4)], ckr_v)
    ld_c = [local(cc_hbm.at[pl.ds(128 * h, 128)], kc.at[0, h, pl.ds(0, 128)]) for h in range(2)]
    ld_tbl = local(tbl_hbm, tbl_v)
    ld_x = local(x_hbm, x_v.at[pl.ds(0, TOK)])
    ld_dkv = local(wdkv_hbm, wdkv_v)
    ld_small = [local(wt_hbm, wt_s), local(g_hbm, g_v)]
    ld_uk = local(wuk_hbm, wuk_v)
    ld_q = [local(wq_hbm.at[:, pl.ds(g * GCOLS, GCOLS)], wq_v.at[g]) for g in range(NGROUP)]
    ld_uv = local(wuv_hbm, wuv_v)
    ld_o = local(wo_hbm, wo_v)

    x_v[pl.ds(TOK, TOK), :] = jnp.zeros((TOK, DM), BF)
    for b in range(NBLK):
        ob_s[b, pl.ds(TOK, TOK), :] = jnp.zeros((TOK, GROUP * ND), BF)
    for pr in range(NH // 2):
        qn_s[pr, pl.ds(0, TOK), pl.ds(ND, ND)] = jnp.zeros((TOK, ND), BF)
        qn_s[pr, pl.ds(TOK, TOK), pl.ds(0, ND)] = jnp.zeros((TOK, ND), BF)
    lane = lax.broadcasted_iota(jnp.int32, (TOK, 128), 1)
    low = lane < RD

    ld_kr.wait()
    for h in range(2):
        kr = ckr_v[pl.ds(2 * h, 2)].reshape(128, RD)
        kc[0, h, pl.ds(128, 16), :] = jnp.concatenate([kr[16 * u:16 * u + 16] for u in range(8)], axis=-1)

    def half_of(c, h):
        return kc.at[c] if h is None else kc.at[c, h]

    def flow(name):
        if name in FLOWS:
            sc, sh, tc, th, d = FLOWS[name]
            src, dst, s_sem, r_sem = half_of(sc, sh), half_of(tc, th), send_sem.at[0], recv_sem.at[tc]
        else:
            ss, ts, d, r = NEWS[name]
            src, dst, s_sem, r_sem = nc.at[ss], nc.at[ts], send_sem.at[1], recv_sem.at[r]
        return pltpu.make_async_remote_copy(src_ref=src, dst_ref=dst, send_sem=s_sem, recv_sem=r_sem,
                                            device_id=(peer[d],), device_id_type=MESH)

    def sends(*names):
        for name in names:
            flow(name).start()

    def arrive(c):
        with scope(f"wait_c{c}"):
            pltpu.make_async_copy(kc.at[c], kc.at[c], recv_sem.at[c]).wait()

    def arrive_new(r):
        first, n = {8: (1, 2), 10: (3, 1), 9: (4, 4)}[r]
        with scope(f"wait_n{r}"):
            pltpu.make_async_copy(nc.at[pl.ds(first, n)], nc.at[pl.ds(first, n)], recv_sem.at[r]).wait()

    with scope("tables"):
        ld_tbl.wait()
        k_lane = lax.rem(lane, 32)
        freq = jnp.zeros((TOK, 128), F32)
        for k, f in enumerate(INV_FREQ):
            freq = jnp.where(k_lane == k, f, freq)
        n_pages = jnp.sum(jnp.where(tbl_v[0:1] >= 0, 1.0, 0.0), axis=-1, keepdims=True)
        pos = lax.broadcasted_iota(jnp.int32, (TOK, 128), 0).astype(F32) + jnp.broadcast_to(n_pages * TOK, (TOK, 128))
        ang = pos * freq
        cos_t = jnp.cos(ang)
        sin_t = jnp.sin(ang)
        sin_t = jnp.where(lax.rem(lane, 64) < 32, -sin_t, sin_t)

    def rope2(v64):
        v = jnp.concatenate([v64, v64], axis=-1)
        return v * cos_t + pltpu.roll(v, 32, 1) * sin_t

    with scope("barrier"):
        pl.semaphore_wait(barrier, 3)
    pl.semaphore_signal(diag_sem, inc=1, device_id=(peer["x"],), device_id_type=MESH)
    with scope("send0"):
        for cp in ld_c:
            cp.wait()
        sends("x0", "y1", "p0", "x1", "y0")

    with scope("mult"):
        tbl = tbl_v[...]
        ids = (tbl[0:1] * 4 + tbl[1:2]).astype(F32)
        ids_col = jnp.transpose(jnp.broadcast_to(ids, (128, 256)))
        seg = lax.div(lax.broadcasted_iota(jnp.int32, (1, 256), 1), 64)
        flips = {0: 0, 1: fp, 2: fx, 4: fy, 3: fp + fx, 5: fp + fy, 6: fx + fy, 7: fp + fx + fy}
        for c, ((ra, ha), (rb, hb)) in enumerate(CHUNKS):
            pa = (me + flips[ra]) * 4 + 2 * ha
            pb = (me + flips[rb]) * 4 + 2 * hb
            want = jnp.where(seg == 0, pa, jnp.where(seg == 1, pa + 1, jnp.where(seg == 2, pb, pb + 1))).astype(F32)
            parts = []
            for t in range(2):
                hit = jnp.where(ids_col == want[:, t * 128:(t + 1) * 128], 1.0, 0.0)
                parts.append(jnp.sum(hit, axis=0, keepdims=True))
            cnt = jnp.concatenate(parts, axis=-1)
            bias_s[c] = jnp.where(cnt > 0.0, jnp.log2(jnp.maximum(cnt, 1.0)), -jnp.inf)

    with scope("newlat"):
        ld_x.wait()
        ld_dkv.wait()
        for cp in ld_small:
            cp.wait()
        kv = lax.dot_general(x_v[pl.ds(0, TOK), :], wdkv_v[...], (((1,), (1,)), ((), ())), preferred_element_type=F32)
        latp = kv[:, :LAT]
        inv_rms = lax.rsqrt(jnp.mean(latp * latp, axis=-1, keepdims=True) + EPS)
        nc[0, pl.ds(0, TOK), :] = (latp * inv_rms * g_v[...].astype(F32).reshape(1, LAT)).astype(BF)
        kr_dup = rope2(kv[:, LAT:])
        kr_low = jnp.where(low, kr_dup, 0.0).astype(BF)
        for u in range(2):
            pair = jnp.where(low[:16], kr_dup[32 * u:32 * u + 16], kr_dup[32 * u + 16:32 * u + 32])
            nc[0, pl.ds(TOK, 16), pl.ds(128 * u, 128)] = pair.astype(BF)
        nc[0, pl.ds(TOK, 16), pl.ds(256, 256)] = jnp.full((16, 256), wt_s[0, 0], jnp.int32).astype(F32).astype(BF)

    r_i = lax.broadcasted_iota(jnp.int32, (256, 256), 0)
    c_i = lax.broadcasted_iota(jnp.int32, (256, 256), 1)
    perm = (r_i == lax.rem(c_i, 16) * 16 + lax.div(c_i, 16)).astype(F32).astype(BF)

    def reorder(src, dst):
        for blk in range(0, 32, 2):
            rows = jnp.concatenate([src[pl.ds((blk + v) * 256, 256), :] for v in range(2)], axis=-1)
            t = jnp.dot(perm, rows, preferred_element_type=F32).astype(BF)
            for v in range(2):
                for h in range(NH):
                    dst[h // 2, pl.ds((blk + v) * 16, 16), pl.ds((h % 2) * ND, ND)] = t[16 * h:16 * h + 16, v * 128:(v + 1) * 128]

    with scope("reorder_uk"):
        ld_uk.wait()
        reorder(wuk_v, wukt)

    def lift(g):
        for pr in range(g * GROUP // 2, (g + 1) * GROUP // 2):
            q_s[pl.ds(pr * 2 * TOK, 2 * TOK), :] = lax.dot_general(
                qn_s[pr], wukt[pr], (((1,), (1,)), ((), ())), preferred_element_type=F32).astype(BF)

    def post(g):
        qg = qraw_s[g % 2].astype(BF).astype(F32)
        for k in range(GROUP):
            h = g * GROUP + k
            qn_s[h // 2, pl.ds((h % 2) * TOK, TOK), pl.ds((h % 2) * ND, ND)] = qg[:, k * HQ:k * HQ + ND].astype(BF)
            qr_s[pl.ds(h * TOK, TOK), :] = rope2(qg[:, k * HQ + ND:(k + 1) * HQ]).astype(BF)

    for g in range(NGROUP):
        with scope(f"waitq{g}"):
            ld_q[g].wait()
        with scope(f"query{g}"):
            qraw_s[g % 2] = jnp.dot(x_v[...], wq_v[g], preferred_element_type=F32)[:TOK]
            if g:
                post(g - 1)
                lift(g - 1)
    with scope("reorder_uv"):
        ld_uv.wait()
        reorder(wuv_v, wuvt)

    NT = (((1,), (1,)), ((), ()))
    row_tok = lax.rem(lax.broadcasted_iota(jnp.int32, (BLK, TOK), 0), TOK)
    causal = lax.broadcasted_iota(jnp.int32, (BLK, TOK), 1) <= row_tok
    lane16 = lax.broadcasted_iota(jnp.int32, (16, 128), 1) < RD

    def rope_keys(c):
        if c < 0:
            return kr_low
        out = []
        for h in range(2):
            for u in range(4):
                t = kc[c, h, pl.ds(128, 16), pl.ds(128 * u, 128)].astype(F32)
                out += [jnp.where(lane16, t, 0.0), jnp.where(lane16, 0.0, t)]
        return jnp.concatenate(out, axis=0).astype(BF)

    def keys_of(c):
        if c < 0:
            return nc[0, pl.ds(0, TOK), :]
        return jnp.concatenate([kc[c, h, pl.ds(0, 128), :] for h in range(2)], axis=0)

    def scores(c, b, slot, kbd):
        rows = pl.ds(b * BLK, BLK)
        s = lax.dot_general(q_s[rows, :], keys_of(c), NT, preferred_element_type=F32)
        s = s + lax.dot_general(qr_s[rows, :], kbd, NT, preferred_element_type=F32)
        if c < 0:
            s_s[slot, :, :TOK] = s
        else:
            s_s[slot] = s

    def weigh(c, b, slot):
        rows = pl.ds(b * BLK, BLK)
        if c < 0:
            t = jnp.where(causal, s_s[slot, :, :TOK] * SCALE2, -jnp.inf)
            mx = jnp.max(t, axis=-1, keepdims=True)
            p = jnp.exp2(t - mx)
            m_s[rows, :] = jnp.broadcast_to(mx, (BLK, 128))
            l_s[rows, :] = jnp.concatenate([p, jnp.zeros_like(p)], axis=-1)
            p_s[slot, :, :TOK] = p.astype(BF)
            return
        t = s_s[slot] * SCALE2 + bias_s[c]
        mx = jnp.max(jnp.maximum(t[:, :128], t[:, 128:]), axis=-1, keepdims=True)
        m_old = m_s[rows, :]
        m_new = jnp.maximum(m_old, jnp.broadcast_to(mx, (BLK, 128)))
        alpha = jnp.exp2(m_old - m_new)
        p = jnp.exp2(t - jnp.concatenate([m_new, m_new], axis=-1))
        m_s[rows, :] = m_new
        a_s[slot] = alpha
        l_s[rows, :] = l_s[rows, :] * alpha + (p[:, :128] + p[:, 128:])
        p_s[slot] = p.astype(BF)

    def combine(c, b, slot):
        rows = pl.ds(b * BLK, BLK)
        if c < 0:
            o_s[rows, :] = jnp.dot(p_s[slot, :, :TOK], keys_of(c), preferred_element_type=F32)
            return
        a4 = jnp.concatenate([a_s[slot]] * 4, axis=-1)
        o_s[rows, :] = o_s[rows, :] * a4 + jnp.dot(p_s[slot], keys_of(c), preferred_element_type=F32)

    def values(b):
        for pr in range(b * GROUP // 2, (b + 1) * GROUP // 2):
            rows = pl.ds(pr * 2 * TOK, 2 * TOK)
            denom = jnp.sum(l_s[rows, :], axis=-1, keepdims=True)
            ol = (o_s[rows, :] / denom).astype(BF)
            val = jnp.dot(ol, wuvt[pr], preferred_element_type=F32).astype(BF)
            ob_s[b, pl.ds(0, TOK), pl.ds((pr * 2 - b * GROUP) * ND, ND)] = val[:TOK, :ND]
            ob_s[b, pl.ds(0, TOK), pl.ds((pr * 2 - b * GROUP) * ND + ND, ND)] = val[TOK:, ND:]

    def project(b):
        deep = pl.ds(b * GROUP * ND, GROUP * ND)
        for j in range(DM // NB):
            cols = pl.ds(j * NB, NB)
            part = jnp.dot(ob_s[b], wo_v[deep, cols], preferred_element_type=F32)[:TOK]
            if b == 0:
                y_acc[:, cols] = x_v[pl.ds(0, TOK), cols].astype(F32) + part
            elif b < NBLK - 1:
                y_acc[:, cols] = y_acc[:, cols] + part
            else:
                y_v[:, cols] = (y_acc[:, cols] + part).astype(BF)

    def pass_on(which, r, *names):
        @pl.when(core == which)
        def _():
            arrive_new(r)
            sends(*names)

    def before(c):
        if c == -1:
            arrive(2)
            pl.semaphore_wait(diag_sem, 1)
            sends("dy", "dx", "p2", "nx", "ny", "nd", "np")
        elif c == 1:
            arrive(1)
        elif c == 3:
            arrive(3)
        elif c == 4:
            arrive(4)
            sends("p4")
        elif c == 5:
            arrive(5)
        elif c == 6:
            arrive(6)
            sends("p6")
        elif c == 7:
            arrive(7)
            pass_on(1, 8, "n1p", "n2p")

    seq = [(c, b) for c in (-1, 0, 1, 2, 4, 3, 5, 6, 7) for b in range(NBLK)]
    end = len(seq)
    for n in range(end + 4):
        if n < end and seq[n][1] == 0:
            before(seq[n][0])
            kbd = rope_keys(seq[n][0])
        if n == end:
            ld_o.wait()
            pass_on(1, 10, "n3p")
            pass_on(0, 8, "n1p", "n2p")
        if n == end + 3:
            pass_on(0, 10, "n3p")
        with scope(f"attend{seq[n][0] if n < end else 99}") if n < end else contextlib.nullcontext():
            if n < end:
                scores(*seq[n], n % 2, kbd)
            if n == 0:
                post(NGROUP - 1)
                lift(NGROUP - 1)
            if 2 <= n < end + 2:
                combine(*seq[n - 2], n % 2)
            if 1 <= n <= end:
                weigh(*seq[n - 1], (n - 1) % 2)
            if end - NBLK <= n - 3 < end:
                values(seq[n - 3][1])
            if end - NBLK <= n - 4 < end:
                project(seq[n - 4][1])

    arrive_new(9)
    with scope("page"):
        mine = me.astype(F32)
        page = jnp.zeros((TOK, LAT), F32)
        packed = jnp.zeros((16, 256), F32)
        for r in range(8):
            hit = nc[r, pl.ds(TOK, 16), pl.ds(256, 256)].astype(F32) == mine
            packed = jnp.where(hit, nc[r, pl.ds(TOK, 16), pl.ds(0, 256)].astype(F32), packed)
            hit = jnp.concatenate([jnp.concatenate([hit] * 2, axis=-1)] * 4, axis=0)
            page = jnp.where(hit, nc[r, pl.ds(0, TOK), :].astype(F32), page)
        pc_v[...] = page.astype(BF)
        packed = packed.astype(BF)
        for u in range(4):
            pk_v[pl.ds(16 * u, 16), :] = packed[:, RD * u:RD * (u + 1)]
    with scope("final_wait"):
        pltpu.make_async_copy(kc.at[pl.ds(0, 7)], kc.at[pl.ds(0, 7)], send_sem.at[0]).wait()
        pltpu.make_async_copy(nc.at[pl.ds(0, 7)], nc.at[pl.ds(0, 7)], send_sem.at[1]).wait()


def finish_body(y_v, cc_v, ckr_v, pc_v, pk_v, y_hbm, cco_hbm, ckro_hbm, sem):
    copies = [
        pltpu.make_async_copy(src, dst, sem.at[n]) for n, (src, dst) in enumerate([
            (y_v, y_hbm),
            (cc_v.at[pl.ds(0, 4)], cco_hbm.at[pl.ds(0, 4)]),
            (pc_v, cco_hbm.at[4]),
            (ckr_v.at[pl.ds(0, 4)], ckro_hbm.at[pl.ds(0, 4)]),
            (pk_v, ckro_hbm.at[4]),
        ])
    ]
    for cp in copies:
        cp.start()
    for cp in copies:
        cp.wait()


def finish(y, cc, ckr, pc, pk):
    return pl.pallas_call(
        finish_body,
        name="mla_finish",
        out_shape=(
            jax.ShapeDtypeStruct((TOK, DM), BF),
            jax.ShapeDtypeStruct((5, TOK, LAT), BF),
            jax.ShapeDtypeStruct((5, TOK, RD), BF),
        ),
        in_specs=[pl.BlockSpec(memory_space=pltpu.VMEM)] * 5,
        out_specs=(pl.BlockSpec(memory_space=pl.ANY),) * 3,
        scratch_shapes=[pltpu.SemaphoreType.DMA((5,))],
        compiler_params=pltpu.CompilerParams(vmem_limit_bytes=4 * 1024 * 1024),
    )(y, cc, ckr, pc, pk)


def fused(*args):
    dma = pltpu.SemaphoreType.DMA
    args = [pltpu.with_memory_space_constraint(a, pltpu.HBM) for a in args]
    return pl.pallas_call(
        body,
        name="mla_prefill",
        out_shape=(
            jax.ShapeDtypeStruct((TOK, DM), BF),
            jax.ShapeDtypeStruct((TOK, LAT), BF),
            jax.ShapeDtypeStruct((TOK, RD), BF),
        ),
        in_specs=[pl.BlockSpec(memory_space=pltpu.HBM)] * len(args),
        out_specs=(pl.BlockSpec(memory_space=pltpu.VMEM),) * 3,
        scratch_shapes=[
            pltpu.VMEM((2 * TOK, DM), BF),
            pltpu.VMEM((2, 256), jnp.int32),
            pltpu.SMEM((1, 2), jnp.int32),
            pltpu.VMEM((4, TOK, RD), BF),
            pltpu.VMEM((NGROUP, DM, GCOLS), BF),
            pltpu.VMEM((LAT + RD, DM), BF),
            pltpu.VMEM((LAT,), BF),
            pltpu.VMEM((LAT * NH, ND), BF),
            pltpu.VMEM((LAT * NH, ND), BF),
            pltpu.VMEM((DM, DM), BF),
            pltpu.VMEM((NBLK, 2 * TOK, GROUP * ND), BF),
            pltpu.VMEM((TOK, DM), F32),
            pltpu.VMEM((8, 2, HALF, LAT), BF),
            pltpu.VMEM((8, NEWR, LAT), BF),
            pltpu.VMEM((NH // 2, LAT, 2 * ND), BF),
            pltpu.VMEM((NH // 2, LAT, 2 * ND), BF),
            pltpu.VMEM((ROWS, LAT), BF),
            pltpu.VMEM((2, TOK, GCOLS), F32),
            pltpu.VMEM((NH // 2, 2 * TOK, 2 * ND), BF),
            pltpu.VMEM((ROWS, 128), BF),
            pltpu.VMEM((2, BLK, 256), F32),
            pltpu.VMEM((2, BLK, 256), BF),
            pltpu.VMEM((2, BLK, 128), F32),
            pltpu.VMEM((ROWS, LAT), F32),
            pltpu.VMEM((ROWS, 128), F32),
            pltpu.VMEM((ROWS, 128), F32),
            pltpu.VMEM((8, 1, 256), F32),
            dma((15,)),
            dma((2,)),
            dma((11,)),
            pltpu.SemaphoreType.REGULAR,
        ],
        compiler_params=pltpu.CompilerParams(collective_id=0, has_side_effects=True, vmem_limit_bytes=50 * 1024 * 1024),
    )(*args)


def solution(mesh):
    def device_step(hidden, pre_len, pre_table, wr_table, cache_c, cache_kr, w_q, w_dkv, g_kv, w_uk, w_uv, w_o):
        y, pc, pk = fused(
            hidden.reshape(TOK, DM), pre_table.reshape(256, 2).T, wr_table.reshape(1, 2), cache_c.reshape(5 * TOK, LAT), cache_kr[0],
            w_q, w_dkv.T, g_kv, w_uk.reshape(LAT * NH, ND), w_uv.reshape(LAT * NH, ND), w_o)
        y, c_out, kr_out = finish(y, cache_c[0], cache_kr[0], pc, pk)
        return y[None], c_out[None], kr_out[None]

    row = P("pool")
    rep = P()
    return jax.shard_map(device_step, mesh=mesh, in_specs=(row,) * 6 + (rep,) * 6, out_specs=(row, row, row), check_vma=False)
```

```python
import contextlib
import math

import jax
import jax.numpy as jnp
import numpy as np
from jax import lax
from jax.experimental import pallas as pl
from jax.experimental.pallas import tpu as pltpu
from jax.sharding import PartitionSpec as P

BF = jnp.bfloat16
PROF = False
F32 = jnp.float32
MESH = pl.DeviceIdType.MESH

TOK = 64
DM = 2048
NH = 16
LAT = 512
RD = 64
ND = 128
HQ = ND + RD
ROWS = NH * TOK
EPS = 1e-6
GROUP = 4
GCOLS = GROUP * HQ
NB = 512
NGROUP = NH // GROUP
BLK = 256
NBLK = ROWS // BLK
SCALE2 = float((ND + RD) ** -0.5 * math.log2(math.e))
INV_FREQ = [float(np.float32(10000.0 ** (-k / 32.0))) for k in range(32)]

CHUNKS = (
    ((0, 0), (0, 1)),
    ((1, 0), (1, 1)),
    ((2, 0), (4, 1)),
    ((3, 0), (5, 1)),
    ((2, 1), (4, 0)),
    ((3, 1), (5, 0)),
    ((6, 0), (6, 1)),
    ((7, 0), (7, 1)),
)
HALF = 128 + 16
NEWR = TOK + 16

FLOWS = {
    "x0": (0, 0, 2, 0, "x"),
    "x1": (0, 1, 4, 0, "x"),
    "y1": (0, 1, 2, 1, "y"),
    "y0": (0, 0, 4, 1, "y"),
    "p0": (0, None, 1, None, "p"),
    "dy": (2, 0, 6, 0, "y"),
    "dx": (2, 1, 6, 1, "x"),
    "p2": (2, None, 3, None, "p"),
    "p4": (4, None, 5, None, "p"),
    "p6": (6, None, 7, None, "p"),
}
NEWS = {
    "nx": (0, 1, 1, "x", 1, 8),
    "ny": (0, 2, 1, "y", 1, 8),
    "np": (0, 3, 1, "p", 1, 11),
    "n1p": (1, 4, 1, "p", 1, 9),
    "n2p": (2, 5, 1, "p", 1, 9),
    "nd": (0, 6, 1, "d", 2, 10),
    "ndp": (3, 7, 1, "d", 2, 10),
    "n6p": (6, 6, 2, "p", 2, 10),
}


def scope(name):
    return jax.named_scope(name) if PROF else contextlib.nullcontext()


def body(x_hbm, tbl_hbm, wt_hbm, cc_hbm, ckr_hbm, wq_hbm, wdkv_hbm, g_hbm, wuk_hbm, wuv_hbm, wo_hbm,
         y_v, pc_v, pk_v,
         x_v, tbl_v, wt_s, ckr_v, wq_v, wdkv_v, g_v, wuk_v, wuv_v, wo_v, ob_s, y_acc,
         kc, nc, wukt, wuvt, q_s, qraw_s, qn_s, qr_s, s_s, p_s, a_s, o_s, m_s, l_s, bias_s,
         loc_sem, send_sem, recv_sem, diag_sem):
    me = lax.axis_index("pool")
    core = lax.rem(me, 2)
    cx = lax.rem(lax.div(me, 2), 2)
    cy = lax.div(me, 4)
    fp = 1 - 2 * core
    fx = 2 - 4 * cx
    fy = 4 - 8 * cy
    peer = {"p": me + fp, "x": me + fx, "y": me + fy, "d": me + fx + fy}

    barrier = pltpu.get_barrier_semaphore()
    for d in ("x", "y", "p"):
        pl.semaphore_signal(barrier, inc=1, device_id=(peer[d],), device_id_type=MESH)

    n_loc = [0]

    def local(src, dst):
        cp = pltpu.make_async_copy(src, dst, loc_sem.at[n_loc[0]])
        n_loc[0] += 1
        cp.start()
        return cp

    ld_kr = local(ckr_hbm.at[pl.ds(0, 4)], ckr_v)
    ld_c = [local(cc_hbm.at[pl.ds(128 * h, 128)], kc.at[0, h, pl.ds(0, 128)]) for h in range(2)]
    ld_tbl = local(tbl_hbm, tbl_v)
    ld_x = local(x_hbm, x_v.at[pl.ds(0, TOK)])
    ld_dkv = local(wdkv_hbm, wdkv_v)
    ld_small = [local(wt_hbm, wt_s), local(g_hbm, g_v)]
    ld_uk = local(wuk_hbm, wuk_v)
    ld_q = [local(wq_hbm.at[:, pl.ds(g * GCOLS, GCOLS)], wq_v.at[g]) for g in range(NGROUP)]
    ld_uv = local(wuv_hbm, wuv_v)
    ld_o = local(wo_hbm, wo_v)

    x_v[pl.ds(TOK, TOK), :] = jnp.zeros((TOK, DM), BF)
    for b in range(NBLK):
        ob_s[b, pl.ds(TOK, TOK), :] = jnp.zeros((TOK, GROUP * ND), BF)
    for pr in range(NH // 2):
        qn_s[pr, pl.ds(0, TOK), pl.ds(ND, ND)] = jnp.zeros((TOK, ND), BF)
        qn_s[pr, pl.ds(TOK, TOK), pl.ds(0, ND)] = jnp.zeros((TOK, ND), BF)
    lane = lax.broadcasted_iota(jnp.int32, (TOK, 128), 1)
    low = lane < RD

    ld_kr.wait()
    for h in range(2):
        kr = ckr_v[pl.ds(2 * h, 2)].reshape(128, RD)
        kc[0, h, pl.ds(128, 16), :] = jnp.concatenate([kr[16 * u:16 * u + 16] for u in range(8)], axis=-1)

    def half_of(c, h):
        return kc.at[c] if h is None else kc.at[c, h]

    def flow(name):
        if name in FLOWS:
            sc, sh, tc, th, d = FLOWS[name]
            src, dst, s_sem, r_sem = half_of(sc, sh), half_of(tc, th), send_sem.at[0], recv_sem.at[tc]
        else:
            ss, ts, n, d, q, r = NEWS[name]
            src, dst, s_sem, r_sem = nc.at[pl.ds(ss, n)], nc.at[pl.ds(ts, n)], send_sem.at[q], recv_sem.at[r]
        return pltpu.make_async_remote_copy(src_ref=src, dst_ref=dst, send_sem=s_sem, recv_sem=r_sem,
                                            device_id=(peer[d],), device_id_type=MESH)

    def sends(*names):
        for name in names:
            flow(name).start()

    def arrive(c):
        with scope(f"wait_c{c}"):
            pltpu.make_async_copy(kc.at[c], kc.at[c], recv_sem.at[c]).wait()

    def arrive_new(r):
        first, n = {8: (1, 2), 11: (3, 1), 9: (4, 2), 10: (6, 2)}[r]
        with scope(f"wait_n{r}"):
            pltpu.make_async_copy(nc.at[pl.ds(first, n)], nc.at[pl.ds(first, n)], recv_sem.at[r]).wait()

    with scope("tables"):
        ld_tbl.wait()
        k_lane = lax.rem(lane, 32)
        freq = jnp.zeros((TOK, 128), F32)
        for k, f in enumerate(INV_FREQ):
            freq = jnp.where(k_lane == k, f, freq)
        n_pages = jnp.sum(jnp.where(tbl_v[0:1] >= 0, 1.0, 0.0), axis=-1, keepdims=True)
        pos = lax.broadcasted_iota(jnp.int32, (TOK, 128), 0).astype(F32) + jnp.broadcast_to(n_pages * TOK, (TOK, 128))
        ang = pos * freq
        cos_t = jnp.cos(ang)
        sin_t = jnp.sin(ang)
        sin_t = jnp.where(lax.rem(lane, 64) < 32, -sin_t, sin_t)

    def rope2(v64):
        v = jnp.concatenate([v64, v64], axis=-1)
        return v * cos_t + pltpu.roll(v, 32, 1) * sin_t

    with scope("barrier"):
        pl.semaphore_wait(barrier, 3)
    @pl.when(core == 1)
    def _():
        pl.semaphore_signal(diag_sem, inc=1, device_id=(peer["x"],), device_id_type=MESH)

    with scope("send0"):
        for cp in ld_c:
            cp.wait()
        sends("x0", "y1", "p0", "x1", "y0")

    with scope("mult"):
        tbl = tbl_v[...]
        ids = (tbl[0:1] * 4 + tbl[1:2]).astype(F32)
        ids_col = jnp.transpose(jnp.broadcast_to(ids, (128, 256)))
        seg = lax.div(lax.broadcasted_iota(jnp.int32, (1, 256), 1), 64)
        flips = {0: 0, 1: fp, 2: fx, 4: fy, 3: fp + fx, 5: fp + fy, 6: fx + fy, 7: fp + fx + fy}
        for c, ((ra, ha), (rb, hb)) in enumerate(CHUNKS):
            pa = (me + flips[ra]) * 4 + 2 * ha
            pb = (me + flips[rb]) * 4 + 2 * hb
            want = jnp.where(seg == 0, pa, jnp.where(seg == 1, pa + 1, jnp.where(seg == 2, pb, pb + 1))).astype(F32)
            parts = []
            for t in range(2):
                hit = jnp.where(ids_col == want[:, t * 128:(t + 1) * 128], 1.0, 0.0)
                parts.append(jnp.sum(hit, axis=0, keepdims=True))
            cnt = jnp.concatenate(parts, axis=-1)
            bias_s[c] = jnp.where(cnt > 0.0, jnp.log2(jnp.maximum(cnt, 1.0)), -jnp.inf)

    with scope("newlat"):
        ld_x.wait()
        ld_dkv.wait()
        for cp in ld_small:
            cp.wait()
        kv = lax.dot_general(x_v[pl.ds(0, TOK), :], wdkv_v[...], (((1,), (1,)), ((), ())), preferred_element_type=F32)
        latp = kv[:, :LAT]
        inv_rms = lax.rsqrt(jnp.mean(latp * latp, axis=-1, keepdims=True) + EPS)
        nc[0, pl.ds(0, TOK), :] = (latp * inv_rms * g_v[...].astype(F32).reshape(1, LAT)).astype(BF)
        kr_dup = rope2(kv[:, LAT:])
        kr_low = jnp.where(low, kr_dup, 0.0).astype(BF)
        for u in range(2):
            pair = jnp.where(low[:16], kr_dup[32 * u:32 * u + 16], kr_dup[32 * u + 16:32 * u + 32])
            nc[0, pl.ds(TOK, 16), pl.ds(128 * u, 128)] = pair.astype(BF)
        nc[0, pl.ds(TOK, 16), pl.ds(256, 256)] = jnp.full((16, 256), wt_s[0, 0], jnp.int32).astype(F32).astype(BF)

    r_i = lax.broadcasted_iota(jnp.int32, (256, 256), 0)
    c_i = lax.broadcasted_iota(jnp.int32, (256, 256), 1)
    perm = (r_i == lax.rem(c_i, 16) * 16 + lax.div(c_i, 16)).astype(F32).astype(BF)

    def reorder(src, dst):
        for blk in range(0, 32, 2):
            rows = jnp.concatenate([src[pl.ds((blk + v) * 256, 256), :] for v in range(2)], axis=-1)
            t = jnp.dot(perm, rows, preferred_element_type=F32).astype(BF)
            for v in range(2):
                for h in range(NH):
                    dst[h // 2, pl.ds((blk + v) * 16, 16), pl.ds((h % 2) * ND, ND)] = t[16 * h:16 * h + 16, v * 128:(v + 1) * 128]

    with scope("reorder_uk"):
        ld_uk.wait()
        reorder(wuk_v, wukt)

    def lift(g):
        for pr in range(g * GROUP // 2, (g + 1) * GROUP // 2):
            q_s[pl.ds(pr * 2 * TOK, 2 * TOK), :] = lax.dot_general(
                qn_s[pr], wukt[pr], (((1,), (1,)), ((), ())), preferred_element_type=F32).astype(BF)

    def post(g):
        qg = qraw_s[g % 2].astype(BF).astype(F32)
        for k in range(GROUP):
            h = g * GROUP + k
            qn_s[h // 2, pl.ds((h % 2) * TOK, TOK), pl.ds((h % 2) * ND, ND)] = qg[:, k * HQ:k * HQ + ND].astype(BF)
            qr_s[pl.ds(h * TOK, TOK), :] = rope2(qg[:, k * HQ + ND:(k + 1) * HQ]).astype(BF)

    for g in range(NGROUP):
        with scope(f"waitq{g}"):
            ld_q[g].wait()
        with scope(f"query{g}"):
            qraw_s[g % 2] = jnp.dot(x_v[...], wq_v[g], preferred_element_type=F32)[:TOK]
            if g:
                post(g - 1)
                lift(g - 1)
    with scope("reorder_uv"):
        ld_uv.wait()
        reorder(wuv_v, wuvt)

    NT = (((1,), (1,)), ((), ()))
    row_tok = lax.rem(lax.broadcasted_iota(jnp.int32, (BLK, TOK), 0), TOK)
    causal = lax.broadcasted_iota(jnp.int32, (BLK, TOK), 1) <= row_tok
    lane16 = lax.broadcasted_iota(jnp.int32, (16, 128), 1) < RD

    def rope_keys(c):
        if c < 0:
            return kr_low
        out = []
        for h in range(2):
            for u in range(4):
                t = kc[c, h, pl.ds(128, 16), pl.ds(128 * u, 128)].astype(F32)
                out += [jnp.where(lane16, t, 0.0), jnp.where(lane16, 0.0, t)]
        return jnp.concatenate(out, axis=0).astype(BF)

    def keys_of(c):
        if c < 0:
            return nc[0, pl.ds(0, TOK), :]
        return jnp.concatenate([kc[c, h, pl.ds(0, 128), :] for h in range(2)], axis=0)

    def scores(c, b, slot, kbd):
        rows = pl.ds(b * BLK, BLK)
        s = lax.dot_general(q_s[rows, :], keys_of(c), NT, preferred_element_type=F32)
        s = s + lax.dot_general(qr_s[rows, :], kbd, NT, preferred_element_type=F32)
        if c < 0:
            s_s[slot, :, :TOK] = s
        else:
            s_s[slot] = s

    def weigh(c, b, slot):
        rows = pl.ds(b * BLK, BLK)
        if c < 0:
            t = jnp.where(causal, s_s[slot, :, :TOK] * SCALE2, -jnp.inf)
            mx = jnp.max(t, axis=-1, keepdims=True)
            p = jnp.exp2(t - mx)
            m_s[rows, :] = jnp.broadcast_to(mx, (BLK, 128))
            l_s[rows, :] = jnp.concatenate([p, jnp.zeros_like(p)], axis=-1)
            p_s[slot, :, :TOK] = p.astype(BF)
            return
        t = s_s[slot] * SCALE2 + bias_s[c]
        mx = jnp.max(jnp.maximum(t[:, :128], t[:, 128:]), axis=-1, keepdims=True)
        m_old = m_s[rows, :]
        m_new = jnp.maximum(m_old, jnp.broadcast_to(mx, (BLK, 128)))
        alpha = jnp.exp2(m_old - m_new)
        p = jnp.exp2(t - jnp.concatenate([m_new, m_new], axis=-1))
        m_s[rows, :] = m_new
        a_s[slot] = alpha
        l_s[rows, :] = l_s[rows, :] * alpha + (p[:, :128] + p[:, 128:])
        p_s[slot] = p.astype(BF)

    def combine(c, b, slot):
        rows = pl.ds(b * BLK, BLK)
        if c < 0:
            o_s[rows, :] = jnp.dot(p_s[slot, :, :TOK], keys_of(c), preferred_element_type=F32)
            return
        a4 = jnp.concatenate([a_s[slot]] * 4, axis=-1)
        o_s[rows, :] = o_s[rows, :] * a4 + jnp.dot(p_s[slot], keys_of(c), preferred_element_type=F32)

    def values(b):
        for pr in range(b * GROUP // 2, (b + 1) * GROUP // 2):
            rows = pl.ds(pr * 2 * TOK, 2 * TOK)
            denom = jnp.sum(l_s[rows, :], axis=-1, keepdims=True)
            ol = (o_s[rows, :] / denom).astype(BF)
            val = jnp.dot(ol, wuvt[pr], preferred_element_type=F32).astype(BF)
            ob_s[b, pl.ds(0, TOK), pl.ds((pr * 2 - b * GROUP) * ND, ND)] = val[:TOK, :ND]
            ob_s[b, pl.ds(0, TOK), pl.ds((pr * 2 - b * GROUP) * ND + ND, ND)] = val[TOK:, ND:]

    def project(b):
        deep = pl.ds(b * GROUP * ND, GROUP * ND)
        for j in range(DM // NB):
            cols = pl.ds(j * NB, NB)
            part = jnp.dot(ob_s[b], wo_v[deep, cols], preferred_element_type=F32)[:TOK]
            if b == 0:
                y_acc[:, cols] = x_v[pl.ds(0, TOK), cols].astype(F32) + part
            elif b < NBLK - 1:
                y_acc[:, cols] = y_acc[:, cols] + part
            else:
                y_v[:, cols] = (y_acc[:, cols] + part).astype(BF)

    def pass_on(which, r, *names):
        @pl.when(core == which)
        def _():
            arrive_new(r)
            sends(*names)

    def before(c):
        if c == -1:
            arrive(2)
            sends("dy", "dx", "p2", "np", "nx", "ny")

            @pl.when(core == 1)
            def _():
                pl.semaphore_wait(diag_sem, 1)
                sends("nd")
        elif c == 1:
            arrive(1)
        elif c == 3:
            arrive(3)
        elif c == 4:
            arrive(4)
            sends("p4")
            pass_on(1, 11, "ndp")
        elif c == 5:
            arrive(5)
        elif c == 6:
            arrive(6)
            sends("p6")
        elif c == 7:
            arrive(7)
            pass_on(1, 8, "n1p", "n2p")

    seq = [(c, b) for c in (-1, 0, 1, 2, 4, 3, 5, 6, 7) for b in range(NBLK)]
    end = len(seq)
    for n in range(end + 4):
        if n < end and seq[n][1] == 0:
            before(seq[n][0])
            kbd = rope_keys(seq[n][0])
        if n == end:
            ld_o.wait()
            pass_on(0, 8, "n1p", "n2p")
        if n == end + 1:
            pass_on(1, 10, "n6p")
        with scope(f"attend{seq[n][0] if n < end else 99}") if n < end else contextlib.nullcontext():
            if n < end:
                scores(*seq[n], n % 2, kbd)
            if n == 0:
                post(NGROUP - 1)
                lift(NGROUP - 1)
            if 2 <= n < end + 2:
                combine(*seq[n - 2], n % 2)
            if 1 <= n <= end:
                weigh(*seq[n - 1], (n - 1) % 2)
            if end - NBLK <= n - 3 < end:
                values(seq[n - 3][1])
            if end - NBLK <= n - 4 < end:
                project(seq[n - 4][1])

    arrive_new(9)
    pass_on(0, 11)
    with scope("page"):
        mine = me.astype(F32)
        page = jnp.zeros((TOK, LAT), F32)
        packed = jnp.zeros((16, 256), F32)
        for r in range(8):
            if r == 6:
                pass_on(0, 10)
            hit = nc[r, pl.ds(TOK, 16), pl.ds(256, 256)].astype(F32) == mine
            packed = jnp.where(hit, nc[r, pl.ds(TOK, 16), pl.ds(0, 256)].astype(F32), packed)
            hit = jnp.concatenate([jnp.concatenate([hit] * 2, axis=-1)] * 4, axis=0)
            page = jnp.where(hit, nc[r, pl.ds(0, TOK), :].astype(F32), page)
        pc_v[...] = page.astype(BF)
        packed = packed.astype(BF)
        for u in range(4):
            pk_v[pl.ds(16 * u, 16), :] = packed[:, RD * u:RD * (u + 1)]
    with scope("final_wait"):
        pltpu.make_async_copy(kc.at[pl.ds(0, 7)], kc.at[pl.ds(0, 7)], send_sem.at[0]).wait()
        pltpu.make_async_copy(nc.at[pl.ds(0, 5)], nc.at[pl.ds(0, 5)], send_sem.at[1]).wait()

        @pl.when(core == 1)
        def _():
            pltpu.make_async_copy(nc.at[pl.ds(0, 4)], nc.at[pl.ds(0, 4)], send_sem.at[2]).wait()


def finish_body(y_v, cc_v, ckr_v, pc_v, pk_v, y_hbm, cco_hbm, ckro_hbm, sem):
    copies = [
        pltpu.make_async_copy(src, dst, sem.at[n]) for n, (src, dst) in enumerate([
            (y_v, y_hbm),
            (cc_v.at[pl.ds(0, 4)], cco_hbm.at[pl.ds(0, 4)]),
            (pc_v, cco_hbm.at[4]),
            (ckr_v.at[pl.ds(0, 4)], ckro_hbm.at[pl.ds(0, 4)]),
            (pk_v, ckro_hbm.at[4]),
        ])
    ]
    for cp in copies:
        cp.start()
    for cp in copies:
        cp.wait()


def finish(y, cc, ckr, pc, pk):
    return pl.pallas_call(
        finish_body,
        name="mla_finish",
        out_shape=(
            jax.ShapeDtypeStruct((TOK, DM), BF),
            jax.ShapeDtypeStruct((5, TOK, LAT), BF),
            jax.ShapeDtypeStruct((5, TOK, RD), BF),
        ),
        in_specs=[pl.BlockSpec(memory_space=pltpu.VMEM)] * 5,
        out_specs=(pl.BlockSpec(memory_space=pl.ANY),) * 3,
        scratch_shapes=[pltpu.SemaphoreType.DMA((5,))],
        compiler_params=pltpu.CompilerParams(vmem_limit_bytes=4 * 1024 * 1024),
    )(y, cc, ckr, pc, pk)


def fused(*args):
    dma = pltpu.SemaphoreType.DMA
    args = [pltpu.with_memory_space_constraint(a, pltpu.HBM) for a in args]
    return pl.pallas_call(
        body,
        name="mla_prefill",
        out_shape=(
            jax.ShapeDtypeStruct((TOK, DM), BF),
            jax.ShapeDtypeStruct((TOK, LAT), BF),
            jax.ShapeDtypeStruct((TOK, RD), BF),
        ),
        in_specs=[pl.BlockSpec(memory_space=pltpu.HBM)] * len(args),
        out_specs=(pl.BlockSpec(memory_space=pltpu.VMEM),) * 3,
        scratch_shapes=[
            pltpu.VMEM((2 * TOK, DM), BF),
            pltpu.VMEM((2, 256), jnp.int32),
            pltpu.SMEM((1, 2), jnp.int32),
            pltpu.VMEM((4, TOK, RD), BF),
            pltpu.VMEM((NGROUP, DM, GCOLS), BF),
            pltpu.VMEM((LAT + RD, DM), BF),
            pltpu.VMEM((LAT,), BF),
            pltpu.VMEM((LAT * NH, ND), BF),
            pltpu.VMEM((LAT * NH, ND), BF),
            pltpu.VMEM((DM, DM), BF),
            pltpu.VMEM((NBLK, 2 * TOK, GROUP * ND), BF),
            pltpu.VMEM((TOK, DM), F32),
            pltpu.VMEM((8, 2, HALF, LAT), BF),
            pltpu.VMEM((8, NEWR, LAT), BF),
            pltpu.VMEM((NH // 2, LAT, 2 * ND), BF),
            pltpu.VMEM((NH // 2, LAT, 2 * ND), BF),
            pltpu.VMEM((ROWS, LAT), BF),
            pltpu.VMEM((2, TOK, GCOLS), F32),
            pltpu.VMEM((NH // 2, 2 * TOK, 2 * ND), BF),
            pltpu.VMEM((ROWS, 128), BF),
            pltpu.VMEM((2, BLK, 256), F32),
            pltpu.VMEM((2, BLK, 256), BF),
            pltpu.VMEM((2, BLK, 128), F32),
            pltpu.VMEM((ROWS, LAT), F32),
            pltpu.VMEM((ROWS, 128), F32),
            pltpu.VMEM((ROWS, 128), F32),
            pltpu.VMEM((8, 1, 256), F32),
            dma((15,)),
            dma((3,)),
            dma((12,)),
            pltpu.SemaphoreType.REGULAR,
        ],
        compiler_params=pltpu.CompilerParams(collective_id=0, has_side_effects=True, vmem_limit_bytes=50 * 1024 * 1024),
    )(*args)


def solution(mesh):
    def device_step(hidden, pre_len, pre_table, wr_table, cache_c, cache_kr, w_q, w_dkv, g_kv, w_uk, w_uv, w_o):
        y, pc, pk = fused(
            hidden.reshape(TOK, DM), pre_table.reshape(256, 2).T, wr_table.reshape(1, 2), cache_c.reshape(5 * TOK, LAT), cache_kr[0],
            w_q, w_dkv.T, g_kv, w_uk.reshape(LAT * NH, ND), w_uv.reshape(LAT * NH, ND), w_o)
        y, c_out, kr_out = finish(y, cache_c[0], cache_kr[0], pc, pk)
        return y[None], c_out[None], kr_out[None]

    row = P("pool")
    rep = P()
    return jax.shard_map(device_step, mesh=mesh, in_specs=(row,) * 6 + (rep,) * 6, out_specs=(row, row, row), check_vma=False)
```
